32 devices in a mesh: dp: 1 (over z), tp: 4 (over y), pp: 8 (over x, core).
Axes of the slice: x: 4, y: 4, z: 1, core: 2. Of those that a mesh axis runs over, the one named last changes fastest.
The devices are a block of a 4x4x8 slice.
Arguments:
- tokens: int32 [4, 128], P('dp')
- labels: int32 [4, 128], P('dp')
- emb_table: bfloat16 [50304, 768], P('tp')
- w_in: bfloat16 [8, 768, 3072], P('pp', None, 'tp')
- w_out: bfloat16 [8, 3072, 768], P('pp', 'tp')
Outputs:
- output 1: float32 [1], P('dp')
- output 2: float32 [8, 768, 3072], P(('dp', 'pp'), None, 'tp')
- output 3: float32 [8, 3072, 768], P(('dp', 'pp'), 'tp')
- output 4: float32 [50304, 768], P(('dp', 'tp'))
All inputs are finite; a program needn't handle non-finite values.
Results may differ from the reference program's by a relative error of at most 0.0122117.
Values are sent between devices in bfloat16 or wider.
A program may use at most 768 MiB of HBM per device.

```python
import jax
import jax.numpy as jnp
from jax import lax

VOCAB_SIZE = 50304
MODEL_DIM = 768
HIDDEN_DIM = 3072
NUM_STAGES = 8
MICRO_BATCHES = 4
SEQ_LEN = 128
NORM_EPS = 1e-6


def setup_inputs(seed: int = 0, part: int = 0) -> dict:
    part_key = jax.random.fold_in(jax.random.key(seed), part)
    key_outer, key_inner, key_rank, key_perm = jax.random.split(part_key, 4)
    id_shape = (MICRO_BATCHES, SEQ_LEN + 1)
    outer_cap = jax.random.randint(key_outer, id_shape, 1, VOCAB_SIZE + 1)
    inner_cap = jax.random.randint(key_inner, id_shape, 1, outer_cap + 1)
    rank_ids = jax.random.randint(key_rank, id_shape, 0, inner_cap)
    vocab_order = jax.random.permutation(key_perm, VOCAB_SIZE)
    id_seq = vocab_order[rank_ids].astype(jnp.int32)
    key_table, key_first, key_second = jax.random.split(jax.random.key(seed + 1), 3)
    emb_table = jax.random.normal(key_table, (VOCAB_SIZE, MODEL_DIM), jnp.float32) * MODEL_DIM ** -0.5
    w_in = jax.random.normal(key_first, (NUM_STAGES, MODEL_DIM, HIDDEN_DIM), jnp.float32) * MODEL_DIM ** -0.5
    w_out = jax.random.normal(key_second, (NUM_STAGES, HIDDEN_DIM, MODEL_DIM), jnp.float32) * (HIDDEN_DIM * NUM_STAGES / 2) ** -0.5
    return {'tokens': id_seq[:, :SEQ_LEN], 'labels': id_seq[:, 1:], 'emb_table': emb_table.astype(jnp.bfloat16), 'w_in': w_in.astype(jnp.bfloat16), 'w_out': w_out.astype(jnp.bfloat16)}


def reference(tokens, labels, emb_table, w_in, w_out):
    vocab_ids = jnp.arange(VOCAB_SIZE, dtype=jnp.int32)

    def layer_fwd(x_act, weights):
        w_one, w_two = weights
        hidden = jnp.dot(x_act, w_one, preferred_element_type=jnp.float32)
        gate_act = jax.nn.gelu(hidden).astype(jnp.bfloat16)
        branch_out = jnp.dot(gate_act, w_two, preferred_element_type=jnp.float32)
        return (x_act.astype(jnp.float32) + branch_out).astype(jnp.bfloat16), (x_act, hidden)

    def layer_bwd(grad_y, saved_act):
        x_act, hidden, w_one, w_two = saved_act
        gate_act, gelu_vjp = jax.vjp(jax.nn.gelu, hidden)
        grad_gate = jnp.dot(grad_y, w_two.T, preferred_element_type=jnp.float32)
        grad_hidden = gelu_vjp(grad_gate)[0].astype(jnp.bfloat16)
        grad_two = jnp.dot(gate_act.astype(jnp.bfloat16).T, grad_y, preferred_element_type=jnp.float32)
        grad_one = jnp.dot(x_act.T, grad_hidden, preferred_element_type=jnp.float32)
        grad_x = (grad_y.astype(jnp.float32) + jnp.dot(grad_hidden, w_one.T, preferred_element_type=jnp.float32)).astype(jnp.bfloat16)
        return grad_x, (grad_one, grad_two)

    def micro_step(carry_in, micro_in):
        loss_sum, acc_one, acc_two, acc_table = carry_in
        tok_row, lab_row = micro_in
        x_first = emb_table[tok_row]
        x_top, saved_fwd = lax.scan(layer_fwd, x_first, (w_in, w_out))
        x_wide = x_top.astype(jnp.float32)
        inv_rms = lax.rsqrt(jnp.mean(x_wide * x_wide, axis=-1, keepdims=True) + NORM_EPS)
        normed = x_wide * inv_rms
        normed_b = normed.astype(jnp.bfloat16)
        logits = jnp.dot(normed_b, emb_table.T, preferred_element_type=jnp.float32)
        log_norm = jax.nn.logsumexp(logits, axis=-1)
        target_hit = lab_row[:, None] == vocab_ids[None, :]
        target_logit = jnp.sum(jnp.where(target_hit, logits, 0.0), axis=-1)
        grad_logits = (jnp.exp(logits - log_norm[:, None]) - target_hit.astype(jnp.float32)).astype(jnp.bfloat16)
        head_grad = jnp.dot(grad_logits.T, normed_b, preferred_element_type=jnp.float32)
        grad_normed = jnp.dot(grad_logits, emb_table, preferred_element_type=jnp.float32)
        grad_top = (inv_rms * (grad_normed - normed * jnp.mean(normed * grad_normed, axis=-1, keepdims=True))).astype(jnp.bfloat16)
        grad_first, stage_grads = lax.scan(layer_bwd, grad_top, (saved_fwd[0], saved_fwd[1], w_in, w_out), reverse=True)
        new_table = (acc_table + head_grad).at[tok_row].add(grad_first.astype(jnp.float32))
        return (loss_sum + jnp.sum(log_norm - target_logit), acc_one + stage_grads[0], acc_two + stage_grads[1], new_table), None

    zero_state = (jnp.zeros((), jnp.float32), jnp.zeros((NUM_STAGES, MODEL_DIM, HIDDEN_DIM), jnp.float32), jnp.zeros((NUM_STAGES, HIDDEN_DIM, MODEL_DIM), jnp.float32), jnp.zeros((VOCAB_SIZE, MODEL_DIM), jnp.float32))
    totals = lax.scan(micro_step, zero_state, (tokens, labels))[0]
    mean_loss = (totals[0] / (MICRO_BATCHES * SEQ_LEN)).reshape(1)
    return mean_loss, totals[1], totals[2], totals[3]
```

```python
import jax
import jax.numpy as jnp
from jax import lax
from jax.sharding import PartitionSpec as P

NORM_EPS = 1e-6


def contract(lhs, rhs, lhs_dim, rhs_dim):
    return lax.dot_general(lhs, rhs, (((lhs_dim,), (rhs_dim,)), ((), ())), preferred_element_type=jnp.float32)


def solution(mesh):
    pp_size = mesh.shape['pp']
    fwd_perm = [(src_stage, src_stage + 1) for src_stage in range(pp_size - 1)]
    bwd_perm = [(src_stage + 1, src_stage) for src_stage in range(pp_size - 1)]

    def device_fn(tokens, labels, emb_table, w_in, w_out):
        num_micro, seq_len = tokens.shape
        vocab_rows, model_dim = emb_table.shape
        num_tok = num_micro * seq_len
        stage_idx = lax.axis_index('pp')
        is_first = stage_idx == 0
        is_last = stage_idx == pp_size - 1
        vocab_base = lax.axis_index('tp') * vocab_rows
        tok_local = tokens - vocab_base
        lab_local = (labels - vocab_base).reshape(num_tok)
        row_ids = jnp.arange(vocab_rows, dtype=jnp.int32)

        w_one = lax.all_gather(w_in[0], 'tp', axis=1, tiled=True)
        w_two = lax.all_gather(w_out[0], 'tp', axis=0, tiled=True)

        owned_ids = (tok_local >= 0) & (tok_local < vocab_rows)
        looked_up = jnp.take(emb_table, jnp.clip(tok_local, 0, vocab_rows - 1), axis=0)
        x_act = lax.psum_scatter(jnp.where(owned_ids[:, :, None], looked_up, jnp.zeros_like(looked_up)), 'tp', scatter_dimension=0)

        x_saved = x_act
        hidden = None
        for tick in range(pp_size):
            x_saved = jnp.where(stage_idx == tick, x_act, x_saved)
            hid = jnp.dot(x_act, w_one, preferred_element_type=jnp.float32)
            branch_out = jnp.dot(jax.nn.gelu(hid).astype(jnp.bfloat16), w_two, preferred_element_type=jnp.float32)
            y_act = (x_act.astype(jnp.float32) + branch_out).astype(jnp.bfloat16)
            if tick < pp_size - 1:
                x_act = lax.ppermute(y_act, 'pp', fwd_perm)
        y_top = lax.psum(jnp.where(is_last, y_act, jnp.zeros_like(y_act)), 'pp')
        hidden = jnp.dot(x_saved, w_one, preferred_element_type=jnp.float32)
        gate_act, gelu_vjp = jax.vjp(jax.nn.gelu, hidden)
        gate_act = gate_act.astype(jnp.bfloat16)
        hidden_cols = w_in.shape[2]

        def to_columns(part):
            part = part.reshape(seq_len, num_micro, hidden_cols)
            return lax.all_to_all(part, 'tp', split_axis=1, concat_axis=0, tiled=True).reshape(num_tok, hidden_cols)

        x_all = lax.all_gather(x_saved, 'tp', axis=0, tiled=True)
        gate_cols = to_columns(gate_act)

        x_wide = y_top.astype(jnp.float32)
        inv_rms = lax.rsqrt(jnp.mean(x_wide * x_wide, axis=-1, keepdims=True) + NORM_EPS)
        normed = x_wide * inv_rms
        normed_all = lax.all_gather(normed.astype(jnp.bfloat16), 'tp', axis=0, tiled=True)

        target_hit = lab_local[:, None] == row_ids[None, :]
        logits = contract(normed_all, emb_table, 1, 1)
        local_max = jnp.max(logits, axis=-1)
        local_sum = jnp.sum(jnp.exp(logits - local_max[:, None]), axis=-1)
        local_target = jnp.sum(jnp.where(target_hit, logits, 0.0), axis=-1)
        stats = lax.all_gather(jnp.stack([local_max + jnp.log(local_sum), local_target]), 'tp')
        log_norm = jax.nn.logsumexp(stats[:, 0], axis=0)
        target_logit = jnp.sum(stats[:, 1], axis=0)
        loss_sum = jnp.sum(log_norm - target_logit)
        grad_logits = (jnp.exp(logits - log_norm[:, None]) - target_hit.astype(jnp.float32)).astype(jnp.bfloat16)
        grad_normed = lax.psum_scatter(contract(grad_logits, emb_table, 1, 0), 'tp', scatter_dimension=0, tiled=True)
        grad_y = (inv_rms * (grad_normed - normed * jnp.mean(normed * grad_normed, axis=-1, keepdims=True))).astype(jnp.bfloat16)

        dy_saved = grad_y
        for tick in range(pp_size):
            here = stage_idx == pp_size - 1 - tick
            dy_saved = jnp.where(here, grad_y, dy_saved)
            grad_hidden = gelu_vjp(contract(grad_y, w_two, 1, 1))[0].astype(jnp.bfloat16)
            dh_saved = grad_hidden if tick == 0 else jnp.where(here, grad_hidden, dh_saved)
            grad_x = (grad_y.astype(jnp.float32) + contract(grad_hidden, w_one, 1, 1)).astype(jnp.bfloat16)
            if tick < pp_size - 1:
                grad_y = lax.ppermute(grad_x, 'pp', bwd_perm)
        dx_all = lax.all_gather(lax.psum(jnp.where(is_first, grad_x, jnp.zeros_like(grad_x)), 'pp'), 'tp', axis=0, tiled=True)
        dy_all = lax.all_gather(dy_saved, 'tp', axis=0, tiled=True)
        dh_cols = to_columns(dh_saved)
        grad_two = contract(gate_cols, dy_all, 0, 0)
        grad_one = contract(x_all, dh_cols, 0, 0)

        one_hot = (tok_local.reshape(num_tok)[:, None] == row_ids[None, :]).astype(jnp.bfloat16)
        grad_table = contract(grad_logits, normed_all, 0, 0) + contract(one_hot, dx_all, 0, 0)
        mean_loss = loss_sum / num_tok
        return mean_loss.reshape(1), grad_one[None], grad_two[None], grad_table

    return jax.shard_map(device_fn, mesh=mesh, in_specs=(P('dp', None), P('dp', None), P('tp', None), P('pp', None, 'tp'), P('pp', 'tp', None)), out_specs=(P('dp'), P(('dp', 'pp'), None, 'tp'), P(('dp', 'pp'), 'tp', None), P(('dp', 'tp'), None)), check_vma=False)
```

```python
import functools

import jax
import jax.numpy as jnp
from jax import lax
from jax.experimental import pallas as pl
from jax.experimental.pallas import tpu as pltpu
from jax.sharding import PartitionSpec as P

NORM_EPS = 1e-6
MESH_ID = pl.DeviceIdType.MESH
GELU_C = 0.7978845608028654
GELU_A = 0.044715
BF16 = jnp.bfloat16
F32 = jnp.float32


def dot_of(lhs, rhs, lhs_dim, rhs_dim):
    return lax.dot_general(lhs, rhs, (((lhs_dim,), (rhs_dim,)), ((), ())), preferred_element_type=F32)


def row_chunk(rows):
    return max(size for size in range(16, 129, 16) if rows % size == 0)


def gelu_pair(hid):
    sq = hid * hid
    tanh = jnp.tanh(GELU_C * (hid + GELU_A * (hid * sq)))
    cdf = 0.5 * (1.0 + tanh)
    slope = cdf + (0.5 * GELU_C) * hid * (1.0 - tanh * tanh) * (1.0 + (3.0 * GELU_A) * sq)
    return hid * cdf, slope


def step_kernel(num_tp, num_pp, tile, x0, lab, e_hbm, w1_hbm, w2_hbm,
                loss_o, dw1_o, dw2_o, g_o, n_o, dx_o,
                x0r, w1s, w2s, x_in, y_buf, a_own, slope, n_all, x_all, a_cols, dy_all, dh_cols, dh_own, dy_in, dx_all,
                logit, stat, dn_send, dn_recv, g_buf,
                w_send, w_recv, p_send, p_recv, tp_send, tp_recv, tree_send, loc):
    rank = lax.axis_index('tp')
    stage = lax.axis_index('pp')
    last = num_pp - 1
    is_first = stage == 0
    is_last = stage == last
    _, seq, dim = x_in.shape
    vocab = e_hbm.shape[0]
    chunk = row_chunk(vocab)
    right = lax.rem(rank + 1, num_tp)
    left = lax.rem(rank + num_tp - 1, num_tp)
    opp = lax.rem(rank + 2, num_tp)
    X0, N, XA, AC, DY, DH, DX, ST, DN = range(9)

    def push(src, dst, ssem, rsem, dev):
        return pltpu.make_async_remote_copy(src_ref=src, dst_ref=dst, send_sem=ssem, recv_sem=rsem, device_id=dev, device_id_type=MESH_ID)

    def swap(kind, src_of, dst, mode):
        for k in range(1, num_tp):
            peer = lax.rem(rank + k, num_tp)
            if mode == 'recv':
                push(dst.at[peer], dst.at[peer], tp_send.at[kind, k], tp_recv.at[kind, peer], {'tp': rank}).wait_recv()
            else:
                copy = push(src_of(peer), dst.at[rank], tp_send.at[kind, k], tp_recv.at[kind, rank], {'tp': peer})
                copy.start() if mode == 'start' else copy.wait_send()

    num_x = num_pp // 2
    chip, core = stage // 2, lax.rem(stage, 2)

    def tree(kind, tid, buf, root, mode):
        root_x, root_c = root // 2, root % 2
        on_core = core == root_c
        partner = (chip * 2 + 1 - root_c)
        plus = lax.rem(chip + 1, num_x) * 2 + root_c
        minus = lax.rem(chip + num_x - 1, num_x) * 2 + root_c
        at_root = jnp.logical_and(on_core, chip == root_x)
        at_next = jnp.logical_and(on_core, jnp.logical_or(chip == root_x, chip == (root_x + 1) % num_x))
        for i in range(num_tp):
            blk = lax.rem(rank + i, num_tp)

            def go(slot, dest):
                copy = push(buf.at[blk], buf.at[blk], tree_send.at[tid, slot, i], tp_recv.at[kind, blk], {'pp': dest})
                copy.start() if mode == 'start' else copy.wait_send()

            if mode == 'start':
                wait = push(buf.at[blk], buf.at[blk], tree_send.at[tid, 0, i], tp_recv.at[kind, blk], {'pp': stage})
                if i == 0:
                    pl.when(stage != root)(wait.wait_recv)
                else:
                    wait.wait_recv()

            @pl.when(at_root)
            def _():
                go(0, minus)

            @pl.when(at_next)
            def _():
                go(1, plus)

            @pl.when(on_core)
            def _():
                go(2, partner)

    barrier = pltpu.get_barrier_semaphore()
    for k in range(1, num_tp):
        pl.semaphore_signal(barrier, inc=1, device_id={'tp': lax.rem(rank + k, num_tp)}, device_id_type=MESH_ID)
    for k in range(1, num_pp):
        pl.semaphore_signal(barrier, inc=1, device_id={'pp': lax.rem(stage + k, num_pp)}, device_id_type=MESH_ID)
    pl.semaphore_wait(barrier, num_tp + num_pp - 2)

    @pl.when(is_first)
    def _():
        swap(X0, lambda peer: x0.at[peer], x0r, 'start')

    own1 = pltpu.make_async_copy(w1_hbm, w1s.at[rank], loc.at[0])
    own2 = pltpu.make_async_copy(w2_hbm, w2s.at[rank], loc.at[1])
    own1.start()
    own2.start()

    def w_copy(idx):
        src, full, who, dev = [
            (w1_hbm, w1s, rank, right), (w2_hbm, w2s, rank, right), (w1_hbm, w1s, rank, left), (w2_hbm, w2s, rank, left),
            (w1s.at[left], w1s, left, right), (w2s.at[right], w2s, right, left)][idx]
        return push(src, full.at[who], w_send.at[idx], w_recv.at[idx], {'tp': dev})

    def w_wait(idx):
        full, who = [(w1s, left), (w2s, left), (w1s, right), (w2s, right), (w1s, opp), (w2s, opp)][idx]
        push(full.at[who], full.at[who], w_send.at[idx], w_recv.at[idx], {'tp': rank}).wait_recv()

    for idx in (0, 3, 1, 2):
        w_copy(idx).start()
    w_wait(0)
    w_copy(4).start()
    w_wait(3)
    w_copy(5).start()

    @pl.when(is_first)
    def _():
        swap(X0, None, x0r, 'recv')
        total = x0[rank].astype(F32)
        for k in range(1, num_tp):
            total = total + x0r[lax.rem(rank + k, num_tp)].astype(F32)
        x_in[0] = total.astype(BF16)

    for idx in (1, 2, 4, 5):
        w_wait(idx)
    own1.wait()
    own2.wait()

    fwd = push(y_buf.at[0], x_in.at[0], p_send.at[0], p_recv.at[0], {'pp': jnp.minimum(stage + 1, last)})
    bwd = push(y_buf.at[1], dy_in.at[0], p_send.at[1], p_recv.at[1], {'pp': jnp.maximum(stage - 1, 0)})

    @pl.when(jnp.logical_not(is_first))
    def _():
        fwd.wait_recv()

    x_act = x_in[0]
    total = x_act.astype(F32)
    for blk in range(num_tp):
        gate, grad = gelu_pair(dot_of(x_act, w1s[blk], 1, 0))
        a_own[blk] = gate.astype(BF16)
        slope[blk] = grad
        total = total + dot_of(a_own[blk], w2s[blk], 1, 0)
    y_buf[0] = total.astype(BF16)

    @pl.when(jnp.logical_not(is_last))
    def _():
        fwd.start()

    def norm_of():
        wide = y_buf[0].astype(F32)
        inv_rms = lax.rsqrt(jnp.mean(wide * wide, axis=-1, keepdims=True) + NORM_EPS)
        return inv_rms, wide * inv_rms

    @pl.when(is_last)
    def _():
        n_all[rank] = norm_of()[1].astype(BF16)
        swap(N, lambda peer: n_all.at[rank], n_all, 'start')

    tree(N, 0, n_all, last, 'start')
    x_all[rank] = x_in[0]
    a_cols[rank] = a_own[rank]
    swap(XA, lambda peer: x_in.at[0], x_all, 'start')
    swap(AC, lambda peer: a_own.at[peer], a_cols, 'start')
    n_out = pltpu.make_async_copy(n_all, n_o, loc.at[0])
    n_out.start()

    num_tok = num_tp * seq
    normed = n_all[...].reshape(num_tok, dim)
    full_tiles, tail = vocab // tile, vocab % tile
    lab_row = lab[...]
    rows_in = lax.broadcasted_iota(jnp.int32, (chunk // 8, 8, num_tok), 0) * 8 + lax.broadcasted_iota(jnp.int32, (chunk // 8, 8, num_tok), 1)

    def stats_of(base, count, carry):
        def one(c, carry):
            top, acc, hit = carry
            row = pl.multiple_of(base + c * chunk, chunk)
            part = logit[pl.ds(row, chunk), :].reshape(chunk // 8, 8, num_tok)
            new = jnp.maximum(top, jnp.max(part, axis=0))
            acc = acc * jnp.exp(top - new) + jnp.sum(jnp.exp(part - new[None]), axis=0)
            hit = hit + jnp.sum(jnp.where(rows_in == (lab_row - row)[None], part, 0.0), axis=0)
            return new, acc, hit
        return lax.fori_loop(0, count // chunk, one, carry)

    def logits_pass(e_buf):
        def fetch(i, size, slot):
            return pltpu.make_async_copy(e_hbm.at[pl.ds(pl.multiple_of(i * tile, 16), size)], e_buf.at[slot, pl.ds(0, size)], loc.at[2 + slot])

        def one(i, carry):
            slot = lax.rem(i, 2)

            @pl.when(i + 1 < full_tiles)
            def _():
                fetch(i + 1, tile, 1 - slot).start()
            fetch(i, tile, slot).wait()
            base = pl.multiple_of(i * tile, 16)
            logit[pl.ds(base, tile), :] = dot_of(e_buf[slot], normed, 1, 1)
            return stats_of(base, tile, carry)

        zero = jnp.zeros((8, num_tok), F32)
        fetch(0, tile, 0).start()
        carry = lax.fori_loop(0, full_tiles, one, (jnp.full((8, num_tok), -jnp.inf, F32), zero, zero))
        if tail:
            base = full_tiles * tile
            last_e = pltpu.make_async_copy(e_hbm.at[pl.ds(base, tail)], e_buf.at[0, pl.ds(0, tail)], loc.at[2])
            last_e.start()
            last_e.wait()
            logit[pl.ds(base, tail), :] = dot_of(e_buf[0, pl.ds(0, tail), :], normed, 1, 1)
            carry = stats_of(base, tail, carry)
        top, acc, hit = carry
        peak = jnp.max(top, axis=0, keepdims=True)
        total = jnp.sum(acc * jnp.exp(top - peak), axis=0, keepdims=True)
        hits = jnp.sum(hit, axis=0, keepdims=True)
        line = lax.broadcasted_iota(jnp.int32, (8, num_tok), 0)
        stat[rank] = jnp.where(line == 0, peak, jnp.where(line == 1, total, hits))

    pl.run_scoped(logits_pass, pltpu.VMEM((2, tile, dim), BF16))

    swap(ST, lambda peer: stat.at[rank], stat, 'start')
    swap(ST, None, stat, 'recv')
    peak = stat[0, 0:1, :]
    for j in range(1, num_tp):
        peak = jnp.maximum(peak, stat[j, 0:1, :])
    total = jnp.zeros_like(peak)
    target = jnp.zeros_like(peak)
    for j in range(num_tp):
        total = total + stat[j, 1:2, :] * jnp.exp(stat[j, 0:1, :] - peak)
        target = target + stat[j, 2:3, :]
    log_norm = peak + jnp.log(total)
    loss = jnp.sum(log_norm - target, axis=1, keepdims=True) / num_tok
    loss_o[...] = jnp.broadcast_to(loss, loss_o.shape)
    norm_rows = jnp.broadcast_to(log_norm, (8, num_tok))

    def grad_tile(base, count, slot):
        def one(c, carry):
            row = pl.multiple_of(base + c * chunk, chunk)
            part = logit[pl.ds(row, chunk), :].reshape(chunk // 8, 8, num_tok)
            hit = jnp.where(rows_in == (lab_row - row)[None], 1.0, 0.0)
            part = jnp.exp(part - norm_rows[None]) - hit
            g_buf[slot, pl.ds(pl.multiple_of(c * chunk, chunk), chunk), :] = part.reshape(chunk, num_tok).astype(BF16)
            return carry
        lax.fori_loop(0, count // chunk, one, 0)

    def grads_pass(e_buf, dn_acc):
        def fetch(base, size, slot):
            return pltpu.make_async_copy(e_hbm.at[pl.ds(base, size)], e_buf.at[slot, pl.ds(0, size)], loc.at[2 + slot])

        def put(base, size, slot):
            return pltpu.make_async_copy(g_buf.at[slot, pl.ds(0, size)], g_o.at[pl.ds(base, size)], loc.at[4 + slot])

        def at(i):
            return pl.multiple_of(i * tile, 16)

        @pl.when(is_last)
        def _():
            dn_acc[...] = jnp.zeros_like(dn_acc)
            fetch(0, tile, 0).start()

        def one(i, carry):
            slot = lax.rem(i, 2)

            @pl.when(i >= 2)
            def _():
                put(at(i - 2), tile, slot).wait()
            grad_tile(at(i), tile, slot)
            put(at(i), tile, slot).start()

            @pl.when(is_last)
            def _():
                @pl.when(i + 1 < full_tiles)
                def _():
                    fetch(at(i + 1), tile, 1 - slot).start()
                fetch(at(i), tile, slot).wait()
                dn_acc[...] += dot_of(g_buf[slot], e_buf[slot], 0, 0)
            return carry

        lax.fori_loop(0, full_tiles, one, 0)
        for i in range(max(full_tiles - 2, 0), full_tiles):
            put(i * tile, tile, i % 2).wait()
        if tail:
            base = full_tiles * tile

            @pl.when(is_last)
            def _():
                fetch(base, tail, 0).start()
            grad_tile(base, tail, 0)
            put(base, tail, 0).start()

            @pl.when(is_last)
            def _():
                fetch(base, tail, 0).wait()
                dn_acc[...] += dot_of(g_buf[0, pl.ds(0, tail), :], e_buf[0, pl.ds(0, tail), :], 0, 0)
            put(base, tail, 0).wait()

        @pl.when(is_last)
        def _():
            for k in range(num_tp):
                dn_send[k] = dn_acc[k * seq:(k + 1) * seq, :].astype(BF16)
            swap(DN, lambda peer: dn_send.at[peer], dn_recv, 'start')
            swap(DN, None, dn_recv, 'recv')
            grad_n = dn_acc[pl.ds(pl.multiple_of(rank * seq, seq), seq), :]
            for k in range(1, num_tp):
                grad_n = grad_n + dn_recv[lax.rem(rank + k, num_tp)].astype(F32)
            inv_rms, unit = norm_of()
            dy_in[0] = (inv_rms * (grad_n - unit * jnp.mean(unit * grad_n, axis=-1, keepdims=True))).astype(BF16)

    pl.run_scoped(grads_pass, pltpu.VMEM((2, tile, dim), BF16), pltpu.VMEM((num_tok, dim), F32))

    @pl.when(jnp.logical_not(is_last))
    def _():
        bwd.wait_recv()

    grad_y = dy_in[0]
    total = grad_y.astype(F32)
    for blk in range(num_tp):
        grad_h = (slope[blk] * dot_of(grad_y, w2s[blk], 1, 1)).astype(BF16)
        dh_own[blk] = grad_h
        total = total + dot_of(grad_h, w1s[blk], 1, 1)
    y_buf[1] = total.astype(BF16)

    @pl.when(jnp.logical_not(is_first))
    def _():
        bwd.start()

    @pl.when(is_first)
    def _():
        dx_all[rank] = y_buf[1]
        swap(DX, lambda peer: y_buf.at[1], dx_all, 'start')
        tree(DX, 1, dx_all, 0, 'start')

    dy_all[rank] = dy_in[0]
    dh_cols[rank] = dh_own[rank]
    swap(DY, lambda peer: dy_in.at[0], dy_all, 'start')
    swap(DH, lambda peer: dh_own.at[peer], dh_cols, 'start')
    for kind, dst in ((XA, x_all), (AC, a_cols), (DY, dy_all), (DH, dh_cols)):
        swap(kind, None, dst, 'recv')

    def weight_grads(dw):
        dw[0] = dot_of(a_cols[...].reshape(num_tok, a_cols.shape[2]), dy_all[...].reshape(num_tok, dim), 0, 0)
        out2 = pltpu.make_async_copy(dw.at[0], dw2_o, loc.at[2])
        out2.start()
        dw[1] = dot_of(x_all[...].reshape(num_tok, dim), dh_cols[...].reshape(num_tok, dh_cols.shape[2]), 0, 0)
        out1 = pltpu.make_async_copy(dw.at[1], dw1_o, loc.at[3])
        out1.start()
        out2.wait()
        out1.wait()

    pl.run_scoped(weight_grads, pltpu.VMEM((2, dim, dim), F32))

    @pl.when(jnp.logical_not(is_first))
    def _():
        tree(DX, 1, dx_all, 0, 'start')
    dx_out = pltpu.make_async_copy(dx_all, dx_o, loc.at[1])
    dx_out.start()

    for idx in range(6):
        w_copy(idx).wait_send()

    @pl.when(is_first)
    def _():
        swap(X0, lambda peer: x0.at[peer], x0r, 'sent')
        swap(DX, lambda peer: y_buf.at[1], dx_all, 'sent')

    @pl.when(is_last)
    def _():
        swap(N, lambda peer: n_all.at[rank], n_all, 'sent')
        swap(DN, lambda peer: dn_send.at[peer], dn_recv, 'sent')

    @pl.when(jnp.logical_not(is_last))
    def _():
        fwd.wait_send()

    @pl.when(jnp.logical_not(is_first))
    def _():
        bwd.wait_send()
    swap(XA, lambda peer: x_in.at[0], x_all, 'sent')
    swap(AC, lambda peer: a_own.at[peer], a_cols, 'sent')
    swap(ST, lambda peer: stat.at[rank], stat, 'sent')
    swap(DY, lambda peer: dy_in.at[0], dy_all, 'sent')
    swap(DH, lambda peer: dh_own.at[peer], dh_cols, 'sent')
    tree(N, 0, n_all, last, 'sent')
    tree(DX, 1, dx_all, 0, 'sent')
    n_out.wait()
    dx_out.wait()


def table_kernel(block, tok, n_all, dx_all, g_ref, out_ref):
    num_tok = tok.shape[1]
    rows = lax.broadcasted_iota(jnp.int32, (block, num_tok), 0) + pl.program_id(0) * block
    one_hot = jnp.where(rows == tok[...], 1.0, 0.0).astype(BF16)
    out_ref[...] = dot_of(g_ref[...], n_all[...], 1, 0) + dot_of(one_hot, dx_all[...], 1, 0)


def solution(mesh):
    num_tp, num_pp = mesh.shape['tp'], mesh.shape['pp']

    def device_fn(tokens, labels, emb_table, w_in, w_out):
        num_micro, seq = tokens.shape
        vocab, dim = emb_table.shape
        cols = w_in.shape[2]
        num_tok = num_micro * seq
        base = lax.axis_index('tp') * vocab
        tok_local = tokens - base
        owned = (tok_local >= 0) & (tok_local < vocab)
        looked_up = jnp.take(emb_table, jnp.clip(tok_local, 0, vocab - 1), axis=0)
        x0 = jnp.where(owned[:, :, None], looked_up, jnp.zeros_like(looked_up))
        lab_row = (labels - base).reshape(1, num_tok)
        tok_row = tok_local.reshape(1, num_tok)
        chunk = row_chunk(vocab)
        tile = chunk * min(10, max(1, vocab // chunk // 3))
        vmem, hbm = pl.BlockSpec(memory_space=pltpu.VMEM), pl.BlockSpec(memory_space=pl.ANY)
        act = (num_tp, seq, dim)
        wide = (num_tp, seq, cols)
        shape = jax.ShapeDtypeStruct
        dma = pltpu.SemaphoreType.DMA
        loss, grad_one, grad_two, g_all, n_all, dx_all = pl.pallas_call(
            functools.partial(step_kernel, num_tp, num_pp, tile),
            out_shape=(shape((8, 128), F32), shape((dim, cols), F32), shape((cols, dim), F32), shape((vocab, num_tok), BF16),
                       shape(act, BF16), shape(act, BF16)),
            in_specs=[vmem, vmem, hbm, hbm, hbm],
            out_specs=(vmem, hbm, hbm, hbm, hbm, hbm),
            scratch_shapes=[
                pltpu.VMEM(act, BF16), pltpu.VMEM((num_tp, dim, cols), BF16), pltpu.VMEM((num_tp, cols, dim), BF16),
                pltpu.VMEM((1, seq, dim), BF16), pltpu.VMEM((2, seq, dim), BF16), pltpu.VMEM(wide, BF16), pltpu.VMEM(wide, F32),
                pltpu.VMEM(act, BF16), pltpu.VMEM(act, BF16), pltpu.VMEM(wide, BF16), pltpu.VMEM(act, BF16), pltpu.VMEM(wide, BF16),
                pltpu.VMEM(wide, BF16), pltpu.VMEM((1, seq, dim), BF16), pltpu.VMEM(act, BF16),
                pltpu.VMEM((vocab, num_tok), F32), pltpu.VMEM((num_tp, 8, num_tok), F32), pltpu.VMEM(act, BF16), pltpu.VMEM(act, BF16),
                pltpu.VMEM((2, tile, num_tok), BF16),
                dma((6,)), dma((6,)), dma((2,)), dma((2,)), dma((9, num_tp)), dma((9, num_tp)), dma((2, 3, num_tp)), dma((6,)),
            ],
            compiler_params=pltpu.CompilerParams(collective_id=0, has_side_effects=True, vmem_limit_bytes=67043328),
            name='step_kernel',
        )(x0, lab_row, emb_table, w_in[0], w_out[0])

        block = chunk * min(10, max(1, vocab // chunk // 3))
        whole = lambda shp: pl.BlockSpec(shp, lambda i: (0, 0))
        grad_table = pl.pallas_call(
            functools.partial(table_kernel, block),
            grid=(pl.cdiv(vocab, block),),
            out_shape=shape((vocab, dim), F32),
            in_specs=[whole((1, num_tok)), whole((num_tok, dim)), whole((num_tok, dim)), pl.BlockSpec((block, num_tok), lambda i: (i, 0))],
            out_specs=pl.BlockSpec((block, dim), lambda i: (i, 0)),
            compiler_params=pltpu.CompilerParams(dimension_semantics=('arbitrary',), vmem_limit_bytes=48 * 1024 * 1024),
            name='table_kernel',
        )(tok_row, n_all.reshape(num_tok, dim), dx_all.reshape(num_tok, dim), g_all)
        return loss[0, :1], grad_one[None], grad_two[None], grad_table

    return jax.shard_map(device_fn, mesh=mesh, in_specs=(P('dp', None), P('dp', None), P('tp', None), P('pp', None, 'tp'), P('pp', 'tp', None)), out_specs=(P('dp'), P(('dp', 'pp'), None, 'tp'), P(('dp', 'pp'), 'tp', None), P(('dp', 'tp'), None)), check_vma=False)
```

```python
import functools

import jax
import jax.numpy as jnp
from jax import lax
from jax.experimental import pallas as pl
from jax.experimental.pallas import tpu as pltpu
from jax.sharding import PartitionSpec as P

NORM_EPS = 1e-6
MESH_ID = pl.DeviceIdType.MESH
GELU_C = 0.7978845608028654
GELU_A = 0.044715
BF16 = jnp.bfloat16
F32 = jnp.float32


def dot_of(lhs, rhs, lhs_dim, rhs_dim):
    return lax.dot_general(lhs, rhs, (((lhs_dim,), (rhs_dim,)), ((), ())), preferred_element_type=F32)


def row_chunk(rows):
    return max(size for size in range(16, 129, 16) if rows % size == 0)


def gelu_pair(hid):
    sq = hid * hid
    tanh = jnp.tanh(GELU_C * (hid + GELU_A * (hid * sq)))
    cdf = 0.5 * (1.0 + tanh)
    slope = cdf + (0.5 * GELU_C) * hid * (1.0 - tanh * tanh) * (1.0 + (3.0 * GELU_A) * sq)
    return hid * cdf, slope


def step_kernel(num_tp, num_pp, tile, half, tok, lab, e_hbm, w1_hbm, w2_hbm,
                loss_o, meta_o, g_o, n_o, dx_o, xa_o, ac_o, dy_o, dh_o,
                x0, x0r, w1s, w2s, x_in, y_buf, a_own, slope, n_all, x_all, a_cols, dy_all, dh_cols, dh_own, dy_in, dx_all,
                logit, stat, dn_send, dn_recv, dn_half, g_buf, key_buf,
                w_send, w_recv, p_send, p_recv, tp_send, tp_recv, tree_send, st_send, st_recv, g_send, g_recv, out_sem, loc):
    rank = lax.axis_index('tp')
    stage = lax.axis_index('pp')
    last = num_pp - 1
    is_first = stage == 0
    is_last = stage == last
    _, seq, dim = x_in.shape
    vocab = e_hbm.shape[0]
    chunk = row_chunk(vocab)
    right = lax.rem(rank + 1, num_tp)
    left = lax.rem(rank + num_tp - 1, num_tp)
    opp = lax.rem(rank + 2, num_tp)
    X0, N, XA, AC, DY, DH, DX, DN = range(8)

    def push(src, dst, ssem, rsem, dev):
        return pltpu.make_async_remote_copy(src_ref=src, dst_ref=dst, send_sem=ssem, recv_sem=rsem, device_id=dev, device_id_type=MESH_ID)

    def swap(kind, src_of, dst, mode):
        for k in range(1, num_tp):
            peer = lax.rem(rank + k, num_tp)
            if mode == 'recv':
                push(dst.at[peer], dst.at[peer], tp_send.at[kind, k], tp_recv.at[kind, peer], {'tp': rank}).wait_recv()
            else:
                copy = push(src_of(peer), dst.at[rank], tp_send.at[kind, k], tp_recv.at[kind, rank], {'tp': peer})
                copy.start() if mode == 'start' else copy.wait_send()

    num_x = num_pp // 2
    chip, core = stage // 2, lax.rem(stage, 2)
    partner = chip * 2 + 1 - core
    is_top = chip == num_x - 1

    def tree(kind, tid, buf, root, mode):
        root_x, root_c = root // 2, root % 2
        on_core = core == root_c
        plus = lax.rem(chip + 1, num_x) * 2 + root_c
        minus = lax.rem(chip + num_x - 1, num_x) * 2 + root_c
        at_root = jnp.logical_and(on_core, chip == root_x)
        at_next = jnp.logical_and(on_core, jnp.logical_or(chip == root_x, chip == (root_x + 1) % num_x))
        for i in range(num_tp):
            blk = lax.rem(rank + i, num_tp)

            def go(slot, dest):
                copy = push(buf.at[blk], buf.at[blk], tree_send.at[tid, slot, i], tp_recv.at[kind, blk], {'pp': dest})
                copy.start() if mode == 'start' else copy.wait_send()

            if mode == 'start':
                wait = push(buf.at[blk], buf.at[blk], tree_send.at[tid, 0, i], tp_recv.at[kind, blk], {'pp': stage})
                if i == 0:
                    pl.when(stage != root)(wait.wait_recv)
                else:
                    wait.wait_recv()

            @pl.when(on_core)
            def _():
                go(2, partner)

            @pl.when(at_root)
            def _():
                go(0, minus)

            @pl.when(at_next)
            def _():
                go(1, plus)

    barrier = pltpu.get_barrier_semaphore()
    for k in range(1, num_tp):
        for pp in (stage, partner):
            pl.semaphore_signal(barrier, inc=1, device_id={'tp': lax.rem(rank + k, num_tp), 'pp': pp}, device_id_type=MESH_ID)
    for k in range(1, num_pp):
        pl.semaphore_signal(barrier, inc=1, device_id={'pp': lax.rem(stage + k, num_pp)}, device_id_type=MESH_ID)
    pl.semaphore_wait(barrier, 2 * (num_tp - 1) + num_pp - 1)

    own1 = pltpu.make_async_copy(w1_hbm, w1s.at[rank], loc.at[0])
    own2 = pltpu.make_async_copy(w2_hbm, w2s.at[rank], loc.at[1])
    own1.start()
    own2.start()

    def w_copy(idx):
        src, full, who, dev = [
            (w1_hbm, w1s, rank, right), (w2_hbm, w2s, rank, right), (w1_hbm, w1s, rank, left), (w2_hbm, w2s, rank, left),
            (w1s.at[left], w1s, left, right), (w2s.at[right], w2s, right, left)][idx]
        return push(src, full.at[who], w_send.at[idx], w_recv.at[idx], {'tp': dev})

    def w_wait(idx):
        full, who = [(w1s, left), (w2s, left), (w1s, right), (w2s, right), (w1s, opp), (w2s, opp)][idx]
        push(full.at[who], full.at[who], w_send.at[idx], w_recv.at[idx], {'tp': rank}).wait_recv()

    for idx in (0, 3, 1, 2):
        w_copy(idx).start()

    num_tok = num_tp * seq
    vocab_base = rank * vocab
    tail_base = (2 * half - 1) * tile
    tail = vocab - tail_base
    tok_row = tok[...] - vocab_base
    lab_row = lab[...] - vocab_base
    rows_in = lax.broadcasted_iota(jnp.int32, (chunk // 8, 8, num_tok), 0) * 8 + lax.broadcasted_iota(jnp.int32, (chunk // 8, 8, num_tok), 1)

    def at(i):
        return pl.multiple_of(i * tile, 16)

    def fetch(e_buf, base, size, slot):
        return pltpu.make_async_copy(e_hbm.at[pl.ds(base, size)], e_buf.at[slot, pl.ds(0, size)], loc.at[2 + slot])

    def sort_tokens():
        key_row = jnp.where(jnp.logical_and(tok_row >= 0, tok_row < vocab), tok_row, 1 << 20).astype(F32)
        lanes = lax.broadcasted_iota(jnp.int32, (1, num_tok), 1).astype(F32)
        step = 128
        key_buf[...] = jnp.transpose(jnp.broadcast_to(key_row, (step, num_tok)))

        def count(b, pos):
            here = key_buf[pl.ds(pl.multiple_of(b * step, step), step), 0:1]
            idx = (lax.broadcasted_iota(jnp.int32, (step, 1), 0) + b * step).astype(F32)
            ahead = jnp.logical_or(here < key_row, jnp.logical_and(here == key_row, idx < lanes))
            return pos + jnp.sum(jnp.where(ahead, 1.0, 0.0), axis=0, keepdims=True)

        def starts(b, acc):
            here = key_buf[pl.ds(pl.multiple_of(b * step, step), step), 0:1]
            return acc + jnp.sum(jnp.where(here < lanes * tile, 1.0, 0.0), axis=0, keepdims=True)

        zero = jnp.zeros((1, num_tok), F32)
        pos_row = lax.fori_loop(0, num_tok // step, count, zero)
        offs = lax.fori_loop(0, num_tok // step, starts, zero)

        def place(b, carry):
            keys, idxs = carry
            here = key_buf[pl.ds(pl.multiple_of(b * step, step), step), 0:1]
            pos = key_buf[pl.ds(pl.multiple_of(b * step, step), step), 1:2]
            idx = (lax.broadcasted_iota(jnp.int32, (step, 1), 0) + b * step).astype(F32)
            mine = pos == lanes
            keys = keys + jnp.sum(jnp.where(mine, here, 0.0), axis=0, keepdims=True)
            return keys, idxs + jnp.sum(jnp.where(mine, idx, 0.0), axis=0, keepdims=True)

        both = jnp.where(lax.broadcasted_iota(jnp.int32, (step, num_tok), 0) == 0, key_row, pos_row)
        key_buf[...] = jnp.transpose(both)
        keys, idxs = lax.fori_loop(0, num_tok // step, place, (zero, zero))
        line = lax.broadcasted_iota(jnp.int32, (8, num_tok), 0)
        meta_o[...] = jnp.where(line == 0, keys, jnp.where(line == 1, idxs, offs)).astype(jnp.int32)

    sort_tokens()

    def lookup_pass(e_buf, acc):
        def tile_of(base, size, slot):
            def one(c, carry):
                row = base + c * chunk
                hot = jnp.where(rows_in == (tok_row - row)[None], 1.0, 0.0)
                g_buf[slot, pl.ds(pl.multiple_of(c * chunk, chunk), chunk), :] = hot.reshape(chunk, num_tok).astype(BF16)
                return carry
            lax.fori_loop(0, size // chunk, one, 0)
            fetch(e_buf, base, size, slot).wait()
            acc[...] += dot_of(g_buf[slot, pl.ds(0, size), :], e_buf[slot, pl.ds(0, size), :], 0, 0)

        acc[...] = jnp.zeros_like(acc)
        fetch(e_buf, 0, tile, 0).start()
        count = 2 * half - 1

        def one(i, carry):
            slot = lax.rem(i, 2)

            @pl.when(i + 1 < count)
            def _():
                fetch(e_buf, at(i + 1), tile, 1 - slot).start()
            tile_of(at(i), tile, slot)
            return carry
        lax.fori_loop(0, count, one, 0)
        fetch(e_buf, tail_base, tail, 0).start()
        tile_of(tail_base, tail, 0)
        for k in range(num_tp):
            x0[k] = acc[k * seq:(k + 1) * seq, :].astype(BF16)

    @pl.when(is_first)
    def _():
        pl.run_scoped(lookup_pass, pltpu.VMEM((2, tile, dim), BF16), pltpu.VMEM((num_tok, dim), F32))
        swap(X0, lambda peer: x0.at[peer], x0r, 'start')

    w_wait(0)
    w_copy(4).start()
    w_wait(3)
    w_copy(5).start()

    @pl.when(is_first)
    def _():
        swap(X0, None, x0r, 'recv')
        total = x0[rank].astype(F32)
        for k in range(1, num_tp):
            total = total + x0r[lax.rem(rank + k, num_tp)].astype(F32)
        x_in[0] = total.astype(BF16)

    for idx in (1, 2, 4, 5):
        w_wait(idx)
    own1.wait()
    own2.wait()

    fwd = push(y_buf.at[0], x_in.at[0], p_send.at[0], p_recv.at[0], {'pp': jnp.minimum(stage + 1, last)})
    bwd = push(y_buf.at[1], dy_in.at[0], p_send.at[1], p_recv.at[1], {'pp': jnp.maximum(stage - 1, 0)})

    @pl.when(jnp.logical_not(is_first))
    def _():
        fwd.wait_recv()

    x_act = x_in[0]
    total = x_act.astype(F32)
    for blk in range(num_tp):
        gate, grad = gelu_pair(dot_of(x_act, w1s[blk], 1, 0))
        a_own[blk] = gate.astype(BF16)
        slope[blk] = grad
        total = total + dot_of(a_own[blk], w2s[blk], 1, 0)
    y_buf[0] = total.astype(BF16)

    @pl.when(jnp.logical_not(is_last))
    def _():
        fwd.start()

    def norm_of():
        wide = y_buf[0].astype(F32)
        inv_rms = lax.rsqrt(jnp.mean(wide * wide, axis=-1, keepdims=True) + NORM_EPS)
        return inv_rms, wide * inv_rms

    @pl.when(is_last)
    def _():
        n_all[rank] = norm_of()[1].astype(BF16)
        swap(N, lambda peer: n_all.at[rank], n_all, 'start')

    tree(N, 0, n_all, last, 'start')
    x_all[rank] = x_in[0]
    a_cols[rank] = a_own[rank]
    swap(XA, lambda peer: x_in.at[0], x_all, 'start')
    swap(AC, lambda peer: a_own.at[peer], a_cols, 'start')
    outs = [(n_all, n_o), (dx_all, dx_o), (x_all, xa_o), (a_cols, ac_o), (dy_all, dy_o), (dh_cols, dh_o)]

    def out_copy(idx):
        return pltpu.make_async_copy(outs[idx][0], outs[idx][1], out_sem.at[idx])

    out_copy(0).start()
    normed = n_all[...].reshape(num_tok, dim)
    base0 = core * (half * tile)
    mine = half - core
    is_odd = core == 1

    def stats_of(base, count, carry):
        def one(c, carry):
            top, acc, hit = carry
            row = pl.multiple_of(base + c * chunk, chunk)
            part = logit[pl.ds(row, chunk), :].reshape(chunk // 8, 8, num_tok)
            new = jnp.maximum(top, jnp.max(part, axis=0))
            acc = acc * jnp.exp(top - new) + jnp.sum(jnp.exp(part - new[None]), axis=0)
            hit = hit + jnp.sum(jnp.where(rows_in == (lab_row - (base0 + row))[None], part, 0.0), axis=0)
            return new, acc, hit
        return lax.fori_loop(0, count // chunk, one, carry)

    slot_of = rank * 2 + core

    def logits_pass(e_buf):
        def finish(carry):
            top, acc, hit = carry
            peak = jnp.max(top, axis=0, keepdims=True)
            total = jnp.sum(acc * jnp.exp(top - peak), axis=0, keepdims=True)
            hits = jnp.sum(hit, axis=0, keepdims=True)
            line = lax.broadcasted_iota(jnp.int32, (8, num_tok), 0)
            stat[slot_of] = jnp.where(line == 0, peak, jnp.where(line == 1, total, hits))

        def one(i, carry):
            slot = lax.rem(i, 2)

            @pl.when(i + 1 < mine)
            def _():
                fetch(e_buf, base0 + at(i + 1), tile, 1 - slot).start()
            fetch(e_buf, base0 + at(i), tile, slot).wait()
            logit[pl.ds(at(i), tile), :] = dot_of(e_buf[slot], normed, 1, 1)
            return stats_of(at(i), tile, carry)

        zero = jnp.zeros((8, num_tok), F32)
        fetch(e_buf, base0, tile, 0).start()
        carry = lax.fori_loop(0, mine, one, (jnp.full((8, num_tok), -jnp.inf, F32), zero, zero))

        @pl.when(is_odd)
        def _():
            slot = (half - 1) % 2
            fetch(e_buf, tail_base, tail, slot).start()
            fetch(e_buf, tail_base, tail, slot).wait()
            logit[pl.ds((half - 1) * tile, tail), :] = dot_of(e_buf[slot, pl.ds(0, tail), :], normed, 1, 1)
            finish(stats_of((half - 1) * tile, tail, carry))

        @pl.when(jnp.logical_not(is_odd))
        def _():
            finish(carry)

    pl.run_scoped(logits_pass, pltpu.VMEM((2, tile, dim), BF16))

    def stats_swap(mode):
        for k in range(num_tp):
            for flip in range(2):
                if k == 0 and flip == 0:
                    continue
                peer = lax.rem(rank + k, num_tp)
                peer_core = core if flip == 0 else 1 - core
                theirs = peer * 2 + peer_core
                if mode == 'recv':
                    push(stat.at[theirs], stat.at[theirs], st_send.at[2 * k + flip], st_recv.at[theirs], {'tp': rank}).wait_recv()
                else:
                    copy = push(stat.at[slot_of], stat.at[slot_of], st_send.at[2 * k + flip], st_recv.at[slot_of],
                                {'tp': peer, 'pp': chip * 2 + peer_core})
                    copy.start() if mode == 'start' else copy.wait_send()

    stats_swap('start')
    stats_swap('recv')
    peak = stat[0, 0:1, :]
    for j in range(1, 2 * num_tp):
        peak = jnp.maximum(peak, stat[j, 0:1, :])
    total = jnp.zeros_like(peak)
    target = jnp.zeros_like(peak)
    for j in range(2 * num_tp):
        total = total + stat[j, 1:2, :] * jnp.exp(stat[j, 0:1, :] - peak)
        target = target + stat[j, 2:3, :]
    log_norm = peak + jnp.log(total)
    loss = jnp.sum(log_norm - target, axis=1, keepdims=True) / num_tok
    loss_o[...] = jnp.broadcast_to(loss, loss_o.shape)
    norm_rows = jnp.broadcast_to(log_norm, (8, num_tok))

    def grad_tile(base, count, slot):
        def one(c, carry):
            row = pl.multiple_of(base + c * chunk, chunk)
            part = logit[pl.ds(row, chunk), :].reshape(chunk // 8, 8, num_tok)
            hit = jnp.where(rows_in == (lab_row - (base0 + row))[None], 1.0, 0.0)
            part = jnp.exp(part - norm_rows[None]) - hit
            g_buf[slot, pl.ds(pl.multiple_of(c * chunk, chunk), chunk), :] = part.reshape(chunk, num_tok).astype(BF16)
            return carry
        lax.fori_loop(0, count // chunk, one, 0)

    def g_copies(i, base, size, slot):
        here, there = g_buf.at[slot, pl.ds(0, size)], g_o.at[pl.ds(base, size)]
        return pltpu.make_async_copy(here, there, loc.at[4 + slot]), push(here, there, g_send.at[slot], g_recv.at[i], {'pp': partner})

    def g_start(i, base, size, slot):
        for copy in g_copies(i, base, size, slot):
            copy.start()

    def g_wait(i, base, size, slot):
        keep, send = g_copies(i, base, size, slot)
        keep.wait()
        send.wait_send()

    def grads_pass(e_buf, dn_acc):
        @pl.when(is_top)
        def _():
            dn_acc[...] = jnp.zeros_like(dn_acc)
            fetch(e_buf, base0, tile, 0).start()

        def one(i, carry):
            slot = lax.rem(i, 2)

            @pl.when(i >= 2)
            def _():
                g_wait(i - 2, base0 + at(i - 2), tile, slot)
            grad_tile(at(i), tile, slot)
            g_start(i, base0 + at(i), tile, slot)

            @pl.when(is_top)
            def _():
                @pl.when(i + 1 < mine)
                def _():
                    fetch(e_buf, base0 + at(i + 1), tile, 1 - slot).start()
                fetch(e_buf, base0 + at(i), tile, slot).wait()
                dn_acc[...] += dot_of(g_buf[slot], e_buf[slot], 0, 0)
            return carry

        lax.fori_loop(0, mine, one, 0)
        final = half - 1
        slot = final % 2

        @pl.when(is_odd)
        def _():
            @pl.when(is_top)
            def _():
                fetch(e_buf, tail_base, tail, slot).start()
            if final >= 2:
                g_wait(final - 2, base0 + (final - 2) * tile, tile, slot)
            grad_tile(final * tile, tail, slot)
            g_start(final, tail_base, tail, slot)

            @pl.when(is_top)
            def _():
                fetch(e_buf, tail_base, tail, slot).wait()
                dn_acc[...] += dot_of(g_buf[slot, pl.ds(0, tail), :], e_buf[slot, pl.ds(0, tail), :], 0, 0)
        to_top = push(dn_send, dn_half, p_send.at[2], p_recv.at[2], {'pp': partner})

        @pl.when(jnp.logical_and(is_top, jnp.logical_not(is_last)))
        def _():
            for k in range(num_tp):
                dn_send[k] = dn_acc[k * seq:(k + 1) * seq, :].astype(BF16)
            to_top.start()

        @pl.when(is_last)
        def _():
            to_top.wait_recv()
            for k in range(num_tp):
                both = dn_acc[k * seq:(k + 1) * seq, :] + dn_half[k].astype(F32)
                dn_acc[k * seq:(k + 1) * seq, :] = both
                dn_send[k] = both.astype(BF16)
            swap(DN, lambda peer: dn_send.at[peer], dn_recv, 'start')
            swap(DN, None, dn_recv, 'recv')
            grad_n = dn_acc[pl.ds(pl.multiple_of(rank * seq, seq), seq), :]
            for k in range(1, num_tp):
                grad_n = grad_n + dn_recv[lax.rem(rank + k, num_tp)].astype(F32)
            inv_rms, unit = norm_of()
            dy_in[0] = (inv_rms * (grad_n - unit * jnp.mean(unit * grad_n, axis=-1, keepdims=True))).astype(BF16)

    pl.run_scoped(grads_pass, pltpu.VMEM((2, tile, dim), BF16), pltpu.VMEM((num_tok, dim), F32))

    @pl.when(jnp.logical_not(is_last))
    def _():
        bwd.wait_recv()

    dy_all[rank] = dy_in[0]
    swap(DY, lambda peer: dy_in.at[0], dy_all, 'start')
    grad_y = dy_in[0]
    total = grad_y.astype(F32)
    for blk in range(num_tp):
        grad_h = (slope[blk] * dot_of(grad_y, w2s[blk], 1, 1)).astype(BF16)
        dh_own[blk] = grad_h
        total = total + dot_of(grad_h, w1s[blk], 1, 1)
    y_buf[1] = total.astype(BF16)

    @pl.when(jnp.logical_not(is_first))
    def _():
        bwd.start()

    @pl.when(is_first)
    def _():
        dx_all[rank] = y_buf[1]
        swap(DX, lambda peer: y_buf.at[1], dx_all, 'start')

    dh_cols[rank] = dh_own[rank]
    swap(DH, lambda peer: dh_own.at[peer], dh_cols, 'start')

    tree(DX, 1, dx_all, 0, 'start')
    out_copy(1).start()
    for idx, kind, dst in ((2, XA, x_all), (3, AC, a_cols), (4, DY, dy_all), (5, DH, dh_cols)):
        swap(kind, None, dst, 'recv')
        out_copy(idx).start()

    for idx in range(6):
        w_copy(idx).wait_send()

    @pl.when(is_first)
    def _():
        swap(X0, lambda peer: x0.at[peer], x0r, 'sent')
        swap(DX, lambda peer: y_buf.at[1], dx_all, 'sent')

    @pl.when(is_last)
    def _():
        swap(N, lambda peer: n_all.at[rank], n_all, 'sent')
        swap(DN, lambda peer: dn_send.at[peer], dn_recv, 'sent')

    @pl.when(jnp.logical_and(is_top, jnp.logical_not(is_last)))
    def _():
        push(dn_send, dn_half, p_send.at[2], p_recv.at[2], {'pp': partner}).wait_send()

    @pl.when(jnp.logical_not(is_last))
    def _():
        fwd.wait_send()

    @pl.when(jnp.logical_not(is_first))
    def _():
        bwd.wait_send()
    swap(XA, lambda peer: x_in.at[0], x_all, 'sent')
    swap(AC, lambda peer: a_own.at[peer], a_cols, 'sent')
    swap(DY, lambda peer: dy_in.at[0], dy_all, 'sent')
    swap(DH, lambda peer: dh_own.at[peer], dh_cols, 'sent')
    stats_swap('sent')
    tree(N, 0, n_all, last, 'sent')
    tree(DX, 1, dx_all, 0, 'sent')

    final = half - 1
    their_base = (1 - core) * (half * tile)

    @pl.when(is_odd)
    def _():
        if final >= 1:
            g_wait(final - 1, base0 + (final - 1) * tile, tile, (final - 1) % 2)
        g_wait(final, tail_base, tail, final % 2)

    @pl.when(jnp.logical_not(is_odd))
    def _():
        for i in range(max(final - 1, 0), half):
            g_wait(i, base0 + i * tile, tile, i % 2)
    for i in range(final):
        g_copies(i, their_base + i * tile, tile, i % 2)[1].wait_recv()

    @pl.when(is_odd)
    def _():
        g_copies(final, their_base + final * tile, tile, final % 2)[1].wait_recv()

    @pl.when(jnp.logical_not(is_odd))
    def _():
        g_copies(final, tail_base, tail, final % 2)[1].wait_recv()
    for idx in range(6):
        out_copy(idx).wait()


def table_kernel(block, meta, loss_in, n_all, dx_all, g_ref, xa, ac, dy, dh, loss_o, out_ref, dw1_o, dw2_o, dx_wide, acts, dw, sems):
    i = pl.program_id(0)
    num_tok, dim = dx_all.shape
    loads = [pltpu.make_async_copy(src, acts.at[j], sems.at[j]) for j, src in enumerate((ac, dy, xa, dh))]
    stores = [pltpu.make_async_copy(dw.at[j], dst, sems.at[4 + j]) for j, dst in enumerate((dw2_o, dw1_o))]

    @pl.when(i == 0)
    def _():
        for load in loads:
            load.start()
        dx_wide[...] = dx_all[...].astype(F32)
        loss_o[0] = jnp.max(loss_in[...])

    out_ref[...] = dot_of(g_ref[...], n_all[...], 1, 0)

    def add(k, carry):
        row = meta[0, k] - i * block
        out_ref[pl.ds(row, 1), :] += dx_wide[pl.ds(meta[1, k], 1), :]
        return carry
    lax.fori_loop(meta[2, i], meta[2, i + 1], add, 0)

    for j in range(2):
        @pl.when(i == 1 + j)
        def _():
            loads[2 * j].wait()
            loads[2 * j + 1].wait()
            dw[j] = dot_of(acts[2 * j], acts[2 * j + 1], 0, 0)
            stores[j].start()

    @pl.when(i == pl.num_programs(0) - 1)
    def _():
        for store in stores:
            store.wait()


def solution(mesh):
    num_tp, num_pp = mesh.shape['tp'], mesh.shape['pp']

    def device_fn(tokens, labels, emb_table, w_in, w_out):
        num_micro, seq = tokens.shape
        vocab, dim = emb_table.shape
        cols = w_in.shape[2]
        num_tok = num_micro * seq
        chunk = row_chunk(vocab)
        chunks = vocab // chunk
        half = 6 if chunks >= 60 else 2
        tile = chunk * pl.cdiv(chunks, 2 * half)
        vmem, hbm = pl.BlockSpec(memory_space=pltpu.VMEM), pl.BlockSpec(memory_space=pl.ANY)
        act = (num_tp, seq, dim)
        wide = (num_tp, seq, cols)
        shape = jax.ShapeDtypeStruct
        dma = pltpu.SemaphoreType.DMA
        loss, meta, g_all, n_all, dx_all, x_all, a_cols, dy_all, dh_cols = pl.pallas_call(
            functools.partial(step_kernel, num_tp, num_pp, tile, half),
            out_shape=(shape((8, 128), F32), shape((8, num_tok), jnp.int32), shape((vocab, num_tok), BF16),
                       shape(act, BF16), shape(act, BF16), shape(act, BF16), shape(wide, BF16), shape(act, BF16), shape(wide, BF16)),
            in_specs=[vmem, vmem, hbm, hbm, hbm],
            out_specs=(vmem, vmem, hbm, hbm, hbm, hbm, hbm, hbm, hbm),
            scratch_shapes=[
                pltpu.VMEM(act, BF16), pltpu.VMEM(act, BF16), pltpu.VMEM((num_tp, dim, cols), BF16), pltpu.VMEM((num_tp, cols, dim), BF16),
                pltpu.VMEM((1, seq, dim), BF16), pltpu.VMEM((2, seq, dim), BF16), pltpu.VMEM(wide, BF16), pltpu.VMEM(wide, F32),
                pltpu.VMEM(act, BF16), pltpu.VMEM(act, BF16), pltpu.VMEM(wide, BF16), pltpu.VMEM(act, BF16), pltpu.VMEM(wide, BF16),
                pltpu.VMEM(wide, BF16), pltpu.VMEM((1, seq, dim), BF16), pltpu.VMEM(act, BF16),
                pltpu.VMEM((half * tile, num_tok), F32), pltpu.VMEM((2 * num_tp, 8, num_tok), F32),
                pltpu.VMEM(act, BF16), pltpu.VMEM(act, BF16), pltpu.VMEM(act, BF16),
                pltpu.VMEM((2, tile, num_tok), BF16), pltpu.VMEM((num_tok, 128), F32),
                dma((6,)), dma((6,)), dma((3,)), dma((3,)), dma((8, num_tp)), dma((8, num_tp)), dma((2, 3, num_tp)),
                dma((2 * num_tp,)), dma((2 * num_tp,)), dma((2,)), dma((half,)), dma((6,)), dma((6,)),
            ],
            compiler_params=pltpu.CompilerParams(collective_id=0, has_side_effects=True, vmem_limit_bytes=67043328),
            name='step_kernel',
        )(tokens.reshape(1, num_tok), labels.reshape(1, num_tok), emb_table, w_in[0], w_out[0])

        whole = lambda shp: pl.BlockSpec(shp, lambda i, meta: (0, 0))
        flat = lambda arr: arr.reshape(num_tok, arr.shape[2])
        loss, grad_table, grad_one, grad_two = pl.pallas_call(
            functools.partial(table_kernel, tile),
            grid_spec=pltpu.PrefetchScalarGridSpec(
                num_scalar_prefetch=1,
                grid=(pl.cdiv(vocab, tile),),
                in_specs=[whole((8, 128)), whole((num_tok, dim)), whole((num_tok, dim)), pl.BlockSpec((tile, num_tok), lambda i, meta: (i, 0)), hbm, hbm, hbm, hbm],
                out_specs=(pl.BlockSpec(memory_space=pltpu.SMEM), pl.BlockSpec((tile, dim), lambda i, meta: (i, 0)), hbm, hbm),
                scratch_shapes=[pltpu.VMEM((num_tok, dim), F32), pltpu.VMEM((4, num_tok, dim), BF16), pltpu.VMEM((2, dim, dim), F32), dma((6,))],
            ),
            out_shape=(shape((1,), F32), shape((vocab, dim), F32), shape((dim, cols), F32), shape((cols, dim), F32)),
            compiler_params=pltpu.CompilerParams(dimension_semantics=('arbitrary',), vmem_limit_bytes=67043328),
            name='table_kernel',
        )(meta, loss, flat(n_all), flat(dx_all), g_all, flat(x_all), flat(a_cols), flat(dy_all), flat(dh_cols))
        return loss, grad_one[None], grad_two[None], grad_table

    return jax.shard_map(device_fn, mesh=mesh, in_specs=(P('dp', None), P('dp', None), P('tp', None), P('pp', None, 'tp'), P('pp', 'tp', None)), out_specs=(P('dp'), P(('dp', 'pp'), None, 'tp'), P(('dp', 'pp'), 'tp', None), P(('dp', 'tp'), None)), check_vma=False)
```

```python
import functools

import jax
import jax.numpy as jnp
from jax import lax
from jax.experimental import pallas as pl
from jax.experimental.pallas import tpu as pltpu
from jax.sharding import PartitionSpec as P

NORM_EPS = 1e-6
MESH_ID = pl.DeviceIdType.MESH
GELU_C = 0.7978845608028654
GELU_A = 0.044715
BF16 = jnp.bfloat16
F32 = jnp.float32


def dot_of(lhs, rhs, lhs_dim, rhs_dim):
    return lax.dot_general(lhs, rhs, (((lhs_dim,), (rhs_dim,)), ((), ())), preferred_element_type=F32)


def row_chunk(rows):
    return max(size for size in range(16, 129, 16) if rows % size == 0)


def gelu_pair(hid):
    sq = hid * hid
    tanh = jnp.tanh(GELU_C * (hid + GELU_A * (hid * sq)))
    cdf = 0.5 * (1.0 + tanh)
    slope = cdf + (0.5 * GELU_C) * hid * (1.0 - tanh * tanh) * (1.0 + (3.0 * GELU_A) * sq)
    return hid * cdf, slope


def step_kernel(num_tp, num_pp, tile, half, tok, lab, e_hbm, w1_hbm, w2_hbm,
                loss_o, meta_o, g_o, n_o, dx_o, xa_o, ac_o, dy_o, dh_o,
                x0, x0r, w1s, w2s, w1t, w2t, x_in, y_buf, a_own, slope, n_all, x_all, a_cols, dy_all, dh_cols, dh_own, dy_in, dx_all,
                logit, stat, dn_send, dn_recv, dn_half, g_buf, key_buf,
                w_send, w_recv, p_send, p_recv, tp_send, tp_recv, tree_send, st_send, st_recv, g_send, g_recv, out_sem, loc):
    rank = lax.axis_index('tp')
    stage = lax.axis_index('pp')
    last = num_pp - 1
    is_first = stage == 0
    is_last = stage == last
    _, seq, dim = x_in.shape
    vocab = e_hbm.shape[0]
    chunk = row_chunk(vocab)
    right = lax.rem(rank + 1, num_tp)
    left = lax.rem(rank + num_tp - 1, num_tp)
    opp = lax.rem(rank + 2, num_tp)
    X0, N, XA, AC, DY, DH, DX, DN = range(8)

    def push(src, dst, ssem, rsem, dev):
        return pltpu.make_async_remote_copy(src_ref=src, dst_ref=dst, send_sem=ssem, recv_sem=rsem, device_id=dev, device_id_type=MESH_ID)

    def swap(kind, src_of, dst, mode):
        for k in range(1, num_tp):
            peer = lax.rem(rank + k, num_tp)
            if mode == 'recv':
                push(dst.at[peer], dst.at[peer], tp_send.at[kind, k], tp_recv.at[kind, peer], {'tp': rank}).wait_recv()
            else:
                copy = push(src_of(peer), dst.at[rank], tp_send.at[kind, k], tp_recv.at[kind, rank], {'tp': peer})
                copy.start() if mode == 'start' else copy.wait_send()

    num_x = num_pp // 2
    chip, core = stage // 2, lax.rem(stage, 2)
    partner = chip * 2 + 1 - core
    is_top = chip == num_x - 1

    def tree(kind, tid, buf, root, mode):
        root_x, root_c = root // 2, root % 2
        on_core = core == root_c
        plus = lax.rem(chip + 1, num_x) * 2 + root_c
        minus = lax.rem(chip + num_x - 1, num_x) * 2 + root_c
        at_root = jnp.logical_and(on_core, chip == root_x)
        at_next = jnp.logical_and(on_core, jnp.logical_or(chip == root_x, chip == (root_x + 1) % num_x))
        for i in range(num_tp):
            blk = lax.rem(rank + i, num_tp)

            def go(slot, dest):
                copy = push(buf.at[blk], buf.at[blk], tree_send.at[tid, slot, i], tp_recv.at[kind, blk], {'pp': dest})
                copy.start() if mode == 'start' else copy.wait_send()

            if mode == 'start':
                wait = push(buf.at[blk], buf.at[blk], tree_send.at[tid, 0, i], tp_recv.at[kind, blk], {'pp': stage})
                if i == 0:
                    pl.when(stage != root)(wait.wait_recv)
                else:
                    wait.wait_recv()

            @pl.when(on_core)
            def _():
                go(2, partner)

            @pl.when(at_root)
            def _():
                go(0, minus)

            @pl.when(at_next)
            def _():
                go(1, plus)

    barrier = pltpu.get_barrier_semaphore()
    for k in range(1, num_tp):
        for pp in (stage, partner):
            pl.semaphore_signal(barrier, inc=1, device_id={'tp': lax.rem(rank + k, num_tp), 'pp': pp}, device_id_type=MESH_ID)
    for k in range(1, num_pp):
        pl.semaphore_signal(barrier, inc=1, device_id={'pp': lax.rem(stage + k, num_pp)}, device_id_type=MESH_ID)
    pl.semaphore_wait(barrier, 2 * (num_tp - 1) + num_pp - 1)

    own1 = pltpu.make_async_copy(w1_hbm, w1s.at[rank], loc.at[0])
    own2 = pltpu.make_async_copy(w2_hbm, w2s.at[rank], loc.at[1])
    own1.start()
    own2.start()

    def w_copy(idx):
        src, full, who, dev = [
            (w1_hbm, w1s, rank, right), (w2_hbm, w2s, rank, right), (w1_hbm, w1s, rank, left), (w2_hbm, w2s, rank, left),
            (w1s.at[left], w1s, left, right), (w2s.at[right], w2s, right, left)][idx]
        return push(src, full.at[who], w_send.at[idx], w_recv.at[idx], {'tp': dev})

    def w_wait(idx):
        full, who = [(w1s, left), (w2s, left), (w1s, right), (w2s, right), (w1s, opp), (w2s, opp)][idx]
        push(full.at[who], full.at[who], w_send.at[idx], w_recv.at[idx], {'tp': rank}).wait_recv()

    for idx in (0, 3, 1, 2):
        w_copy(idx).start()

    def flip(src, dst, who):
        def one(j, carry):
            part = pl.ds(pl.multiple_of(j * 128, 128), 128)
            dst[who, :, part] = jnp.transpose(src[who, part, :])
            return carry
        lax.fori_loop(0, src.shape[1] // 128, one, 0)

    num_tok = num_tp * seq
    vocab_base = rank * vocab
    tail_base = (2 * half - 1) * tile
    tail = vocab - tail_base
    tok_row = tok[...] - vocab_base
    lab_row = lab[...] - vocab_base
    rows_in = lax.broadcasted_iota(jnp.int32, (chunk // 8, 8, num_tok), 0) * 8 + lax.broadcasted_iota(jnp.int32, (chunk // 8, 8, num_tok), 1)

    def at(i):
        return pl.multiple_of(i * tile, 16)

    def fetch(e_buf, base, size, slot):
        return pltpu.make_async_copy(e_hbm.at[pl.ds(base, size)], e_buf.at[slot, pl.ds(0, size)], loc.at[2 + slot])

    def sort_tokens():
        key_row = jnp.where(jnp.logical_and(tok_row >= 0, tok_row < vocab), tok_row, 1 << 20).astype(F32)
        lanes = lax.broadcasted_iota(jnp.int32, (1, num_tok), 1).astype(F32)
        step = 128
        key_buf[...] = jnp.transpose(jnp.broadcast_to(key_row, (step, num_tok)))

        def count(b, pos):
            here = key_buf[pl.ds(pl.multiple_of(b * step, step), step), 0:1]
            idx = (lax.broadcasted_iota(jnp.int32, (step, 1), 0) + b * step).astype(F32)
            ahead = jnp.logical_or(here < key_row, jnp.logical_and(here == key_row, idx < lanes))
            return pos + jnp.sum(jnp.where(ahead, 1.0, 0.0), axis=0, keepdims=True)

        def starts(b, acc):
            here = key_buf[pl.ds(pl.multiple_of(b * step, step), step), 0:1]
            return acc + jnp.sum(jnp.where(here < lanes * tile, 1.0, 0.0), axis=0, keepdims=True)

        zero = jnp.zeros((1, num_tok), F32)
        pos_row = lax.fori_loop(0, num_tok // step, count, zero)
        offs = lax.fori_loop(0, num_tok // step, starts, zero)

        def place(b, carry):
            keys, idxs = carry
            here = key_buf[pl.ds(pl.multiple_of(b * step, step), step), 0:1]
            pos = key_buf[pl.ds(pl.multiple_of(b * step, step), step), 1:2]
            idx = (lax.broadcasted_iota(jnp.int32, (step, 1), 0) + b * step).astype(F32)
            mine = pos == lanes
            keys = keys + jnp.sum(jnp.where(mine, here, 0.0), axis=0, keepdims=True)
            return keys, idxs + jnp.sum(jnp.where(mine, idx, 0.0), axis=0, keepdims=True)

        both = jnp.where(lax.broadcasted_iota(jnp.int32, (step, num_tok), 0) == 0, key_row, pos_row)
        key_buf[...] = jnp.transpose(both)
        keys, idxs = lax.fori_loop(0, num_tok // step, place, (zero, zero))
        line = lax.broadcasted_iota(jnp.int32, (8, num_tok), 0)
        meta_o[...] = jnp.where(line == 0, keys, jnp.where(line == 1, idxs, offs)).astype(jnp.int32)

    sort_tokens()

    def lookup_pass(e_buf, acc):
        def tile_of(base, size, slot):
            def one(c, carry):
                row = base + c * chunk
                hot = jnp.where(rows_in == (tok_row - row)[None], 1.0, 0.0)
                g_buf[slot, pl.ds(pl.multiple_of(c * chunk, chunk), chunk), :] = hot.reshape(chunk, num_tok).astype(BF16)
                return carry
            lax.fori_loop(0, size // chunk, one, 0)
            fetch(e_buf, base, size, slot).wait()
            acc[...] += dot_of(g_buf[slot, pl.ds(0, size), :], e_buf[slot, pl.ds(0, size), :], 0, 0)

        acc[...] = jnp.zeros_like(acc)
        fetch(e_buf, 0, tile, 0).start()
        count = 2 * half - 1

        def one(i, carry):
            slot = lax.rem(i, 2)

            @pl.when(i + 1 < count)
            def _():
                fetch(e_buf, at(i + 1), tile, 1 - slot).start()
            tile_of(at(i), tile, slot)
            return carry
        lax.fori_loop(0, count, one, 0)
        fetch(e_buf, tail_base, tail, 0).start()
        tile_of(tail_base, tail, 0)
        for k in range(num_tp):
            x0[k] = acc[k * seq:(k + 1) * seq, :].astype(BF16)

    @pl.when(is_first)
    def _():
        pl.run_scoped(lookup_pass, pltpu.VMEM((2, tile, dim), BF16), pltpu.VMEM((num_tok, dim), F32))
        swap(X0, lambda peer: x0.at[peer], x0r, 'start')

    own1.wait()
    own2.wait()
    flip(w1s, w1t, rank)
    flip(w2s, w2t, rank)
    w_wait(0)
    w_copy(4).start()
    w_wait(3)
    w_copy(5).start()
    flip(w1s, w1t, left)
    flip(w2s, w2t, right)

    @pl.when(is_first)
    def _():
        swap(X0, None, x0r, 'recv')
        total = x0[rank].astype(F32)
        for k in range(1, num_tp):
            total = total + x0r[lax.rem(rank + k, num_tp)].astype(F32)
        x_in[0] = total.astype(BF16)

    w_wait(1)
    w_wait(2)
    flip(w2s, w2t, left)
    flip(w1s, w1t, right)
    w_wait(4)
    w_wait(5)

    cols = w1s.shape[2]
    piece = 256 if cols % 256 == 0 and dim % 256 == 0 else 128
    cut = dim // 3 // 128 * 128
    spans = [(0, cut), (cut, dim - cut)] if cut else [(0, dim)]

    def hop(kind, src, dst, part, dest):
        lo, size = spans[part]
        view = (0, slice(None), pl.ds(lo, size))
        return push(src.at[view], dst.at[view], p_send.at[2 * kind + part], p_recv.at[2 * kind + part], {'pp': dest})

    def hops(kind, mode):
        src, dst = (y_buf.at[pl.ds(0, 1)], x_in) if kind == 0 else (y_buf.at[pl.ds(1, 1)], dy_in)
        dest = jnp.minimum(stage + 1, last) if kind == 0 else jnp.maximum(stage - 1, 0)
        return [hop(kind, src, dst, part, dest) for part in range(len(spans))]

    def send_rows(kind, source, acts, mats, active):
        for part, (lo, size) in enumerate(spans):
            for off in range(lo, lo + size, piece):
                total = source[0, :, off:off + piece].astype(F32)
                for blk in range(num_tp):
                    total = total + dot_of(acts[blk], mats[blk, :, off:off + piece], 1, 0)
                y_buf[kind, :, off:off + piece] = total.astype(BF16)

            @pl.when(active)
            def _():
                hops(kind, 'start')[part].start()

    @pl.when(jnp.logical_not(is_first))
    def _():
        for copy in hops(0, 'recv'):
            copy.wait_recv()

    x_act = x_in[0]
    for blk in range(num_tp):
        for off in range(0, cols, piece):
            gate, grad = gelu_pair(dot_of(x_act, w1s[blk, :, off:off + piece], 1, 0))
            a_own[blk, :, off:off + piece] = gate.astype(BF16)
            slope[blk, :, off:off + piece] = grad
    send_rows(0, x_in, a_own, w2s, jnp.logical_not(is_last))

    def norm_of():
        wide = y_buf[0].astype(F32)
        inv_rms = lax.rsqrt(jnp.mean(wide * wide, axis=-1, keepdims=True) + NORM_EPS)
        return inv_rms, wide * inv_rms

    @pl.when(is_last)
    def _():
        n_all[rank] = norm_of()[1].astype(BF16)
        swap(N, lambda peer: n_all.at[rank], n_all, 'start')

    flip(w1s, w1t, opp)
    flip(w2s, w2t, opp)
    tree(N, 0, n_all, last, 'start')
    x_all[rank] = x_in[0]
    a_cols[rank] = a_own[rank]
    swap(XA, lambda peer: x_in.at[0], x_all, 'start')
    swap(AC, lambda peer: a_own.at[peer], a_cols, 'start')
    outs = [(n_all, n_o), (dx_all, dx_o), (x_all, xa_o), (a_cols, ac_o), (dy_all, dy_o), (dh_cols, dh_o)]

    def out_copy(idx):
        return pltpu.make_async_copy(outs[idx][0], outs[idx][1], out_sem.at[idx])

    out_copy(0).start()
    normed = n_all[...].reshape(num_tok, dim)
    base0 = core * (half * tile)
    mine = half - core
    is_odd = core == 1

    def stats_of(base, count, carry):
        def one(c, carry):
            top, acc, hit = carry
            row = pl.multiple_of(base + c * chunk, chunk)
            part = logit[pl.ds(row, chunk), :].reshape(chunk // 8, 8, num_tok)
            new = jnp.maximum(top, jnp.max(part, axis=0))
            acc = acc * jnp.exp(top - new) + jnp.sum(jnp.exp(part - new[None]), axis=0)
            hit = hit + jnp.sum(jnp.where(rows_in == (lab_row - (base0 + row))[None], part, 0.0), axis=0)
            return new, acc, hit
        return lax.fori_loop(0, count // chunk, one, carry)

    slot_of = rank * 2 + core

    def logits_pass(e_buf):
        def finish(carry):
            top, acc, hit = carry
            peak = jnp.max(top, axis=0, keepdims=True)
            total = jnp.sum(acc * jnp.exp(top - peak), axis=0, keepdims=True)
            hits = jnp.sum(hit, axis=0, keepdims=True)
            line = lax.broadcasted_iota(jnp.int32, (8, num_tok), 0)
            stat[slot_of] = jnp.where(line == 0, peak, jnp.where(line == 1, total, hits))

        def one(i, carry):
            slot = lax.rem(i, 2)

            @pl.when(i + 1 < mine)
            def _():
                fetch(e_buf, base0 + at(i + 1), tile, 1 - slot).start()
            fetch(e_buf, base0 + at(i), tile, slot).wait()
            logit[pl.ds(at(i), tile), :] = dot_of(e_buf[slot], normed, 1, 1)
            return stats_of(at(i), tile, carry)

        zero = jnp.zeros((8, num_tok), F32)
        fetch(e_buf, base0, tile, 0).start()
        carry = lax.fori_loop(0, mine, one, (jnp.full((8, num_tok), -jnp.inf, F32), zero, zero))

        @pl.when(is_odd)
        def _():
            slot = (half - 1) % 2
            fetch(e_buf, tail_base, tail, slot).start()
            fetch(e_buf, tail_base, tail, slot).wait()
            logit[pl.ds((half - 1) * tile, tail), :] = dot_of(e_buf[slot, pl.ds(0, tail), :], normed, 1, 1)
            finish(stats_of((half - 1) * tile, tail, carry))

        @pl.when(jnp.logical_not(is_odd))
        def _():
            finish(carry)

    pl.run_scoped(logits_pass, pltpu.VMEM((2, tile, dim), BF16))

    def stats_swap(mode):
        for k in range(num_tp):
            for flip in range(2):
                if k == 0 and flip == 0:
                    continue
                peer = lax.rem(rank + k, num_tp)
                peer_core = core if flip == 0 else 1 - core
                theirs = peer * 2 + peer_core
                if mode == 'recv':
                    push(stat.at[theirs], stat.at[theirs], st_send.at[2 * k + flip], st_recv.at[theirs], {'tp': rank}).wait_recv()
                else:
                    copy = push(stat.at[slot_of], stat.at[slot_of], st_send.at[2 * k + flip], st_recv.at[slot_of],
                                {'tp': peer, 'pp': chip * 2 + peer_core})
                    copy.start() if mode == 'start' else copy.wait_send()

    stats_swap('start')
    stats_swap('recv')
    peak = stat[0, 0:1, :]
    for j in range(1, 2 * num_tp):
        peak = jnp.maximum(peak, stat[j, 0:1, :])
    total = jnp.zeros_like(peak)
    target = jnp.zeros_like(peak)
    for j in range(2 * num_tp):
        total = total + stat[j, 1:2, :] * jnp.exp(stat[j, 0:1, :] - peak)
        target = target + stat[j, 2:3, :]
    log_norm = peak + jnp.log(total)
    loss = jnp.sum(log_norm - target, axis=1, keepdims=True) / num_tok
    loss_o[...] = jnp.broadcast_to(loss, loss_o.shape)
    norm_rows = jnp.broadcast_to(log_norm, (8, num_tok))

    def grad_tile(base, count, slot):
        def one(c, carry):
            row = pl.multiple_of(base + c * chunk, chunk)
            part = logit[pl.ds(row, chunk), :].reshape(chunk // 8, 8, num_tok)
            hit = jnp.where(rows_in == (lab_row - (base0 + row))[None], 1.0, 0.0)
            part = jnp.exp(part - norm_rows[None]) - hit
            g_buf[slot, pl.ds(pl.multiple_of(c * chunk, chunk), chunk), :] = part.reshape(chunk, num_tok).astype(BF16)
            return carry
        lax.fori_loop(0, count // chunk, one, 0)

    def g_copies(i, base, size, slot):
        here, there = g_buf.at[slot, pl.ds(0, size)], g_o.at[pl.ds(base, size)]
        return pltpu.make_async_copy(here, there, loc.at[4 + slot]), push(here, there, g_send.at[slot], g_recv.at[i], {'pp': partner})

    def g_start(i, base, size, slot):
        for copy in g_copies(i, base, size, slot):
            copy.start()

    def g_wait(i, base, size, slot):
        keep, send = g_copies(i, base, size, slot)
        keep.wait()
        send.wait_send()

    def grads_pass(e_buf, dn_acc):
        @pl.when(is_top)
        def _():
            dn_acc[...] = jnp.zeros_like(dn_acc)
            fetch(e_buf, base0, tile, 0).start()

        def one(i, carry):
            slot = lax.rem(i, 2)

            @pl.when(i >= 2)
            def _():
                g_wait(i - 2, base0 + at(i - 2), tile, slot)
            grad_tile(at(i), tile, slot)
            g_start(i, base0 + at(i), tile, slot)

            @pl.when(is_top)
            def _():
                @pl.when(i + 1 < mine)
                def _():
                    fetch(e_buf, base0 + at(i + 1), tile, 1 - slot).start()
                fetch(e_buf, base0 + at(i), tile, slot).wait()
                dn_acc[...] += dot_of(g_buf[slot], e_buf[slot], 0, 0)
            return carry

        lax.fori_loop(0, mine, one, 0)
        final = half - 1
        slot = final % 2

        @pl.when(is_odd)
        def _():
            @pl.when(is_top)
            def _():
                fetch(e_buf, tail_base, tail, slot).start()
            if final >= 2:
                g_wait(final - 2, base0 + (final - 2) * tile, tile, slot)
            grad_tile(final * tile, tail, slot)
            g_start(final, tail_base, tail, slot)

            @pl.when(is_top)
            def _():
                fetch(e_buf, tail_base, tail, slot).wait()
                dn_acc[...] += dot_of(g_buf[slot, pl.ds(0, tail), :], e_buf[slot, pl.ds(0, tail), :], 0, 0)
        to_top = push(dn_send, dn_half, p_send.at[4], p_recv.at[4], {'pp': partner})

        @pl.when(jnp.logical_and(is_top, jnp.logical_not(is_last)))
        def _():
            for k in range(num_tp):
                dn_send[k] = dn_acc[k * seq:(k + 1) * seq, :].astype(BF16)
            to_top.start()

        @pl.when(is_last)
        def _():
            to_top.wait_recv()
            for k in range(num_tp):
                both = dn_acc[k * seq:(k + 1) * seq, :] + dn_half[k].astype(F32)
                dn_acc[k * seq:(k + 1) * seq, :] = both
                dn_send[k] = both.astype(BF16)
            swap(DN, lambda peer: dn_send.at[peer], dn_recv, 'start')
            swap(DN, None, dn_recv, 'recv')
            grad_n = dn_acc[pl.ds(pl.multiple_of(rank * seq, seq), seq), :]
            for k in range(1, num_tp):
                grad_n = grad_n + dn_recv[lax.rem(rank + k, num_tp)].astype(F32)
            inv_rms, unit = norm_of()
            dy_in[0] = (inv_rms * (grad_n - unit * jnp.mean(unit * grad_n, axis=-1, keepdims=True))).astype(BF16)

    pl.run_scoped(grads_pass, pltpu.VMEM((2, tile, dim), BF16), pltpu.VMEM((num_tok, dim), F32))

    @pl.when(jnp.logical_not(is_last))
    def _():
        for copy in hops(1, 'recv'):
            copy.wait_recv()

    dy_all[rank] = dy_in[0]
    swap(DY, lambda peer: dy_in.at[0], dy_all, 'start')
    grad_y = dy_in[0]
    for blk in range(num_tp):
        for off in range(0, cols, piece):
            grad_a = dot_of(grad_y, w2t[blk, :, off:off + piece], 1, 0)
            dh_own[blk, :, off:off + piece] = (slope[blk, :, off:off + piece] * grad_a).astype(BF16)
    send_rows(1, dy_in, dh_own, w1t, jnp.logical_not(is_first))

    @pl.when(is_first)
    def _():
        dx_all[rank] = y_buf[1]
        swap(DX, lambda peer: y_buf.at[1], dx_all, 'start')

    dh_cols[rank] = dh_own[rank]

    @pl.when(chip != 0)
    def _():
        swap(DH, lambda peer: dh_own.at[peer], dh_cols, 'start')

    tree(DX, 1, dx_all, 0, 'start')

    @pl.when(chip == 0)
    def _():
        swap(DH, lambda peer: dh_own.at[peer], dh_cols, 'start')

    out_copy(1).start()
    for idx, kind, dst in ((2, XA, x_all), (3, AC, a_cols), (4, DY, dy_all), (5, DH, dh_cols)):
        swap(kind, None, dst, 'recv')
        out_copy(idx).start()

    for idx in range(6):
        w_copy(idx).wait_send()

    @pl.when(is_first)
    def _():
        swap(X0, lambda peer: x0.at[peer], x0r, 'sent')
        swap(DX, lambda peer: y_buf.at[1], dx_all, 'sent')

    @pl.when(is_last)
    def _():
        swap(N, lambda peer: n_all.at[rank], n_all, 'sent')
        swap(DN, lambda peer: dn_send.at[peer], dn_recv, 'sent')

    @pl.when(jnp.logical_and(is_top, jnp.logical_not(is_last)))
    def _():
        push(dn_send, dn_half, p_send.at[4], p_recv.at[4], {'pp': partner}).wait_send()

    @pl.when(jnp.logical_not(is_last))
    def _():
        for copy in hops(0, 'sent'):
            copy.wait_send()

    @pl.when(jnp.logical_not(is_first))
    def _():
        for copy in hops(1, 'sent'):
            copy.wait_send()
    swap(XA, lambda peer: x_in.at[0], x_all, 'sent')
    swap(AC, lambda peer: a_own.at[peer], a_cols, 'sent')
    swap(DY, lambda peer: dy_in.at[0], dy_all, 'sent')
    swap(DH, lambda peer: dh_own.at[peer], dh_cols, 'sent')
    stats_swap('sent')
    tree(N, 0, n_all, last, 'sent')
    tree(DX, 1, dx_all, 0, 'sent')

    final = half - 1
    their_base = (1 - core) * (half * tile)

    @pl.when(is_odd)
    def _():
        if final >= 1:
            g_wait(final - 1, base0 + (final - 1) * tile, tile, (final - 1) % 2)
        g_wait(final, tail_base, tail, final % 2)

    @pl.when(jnp.logical_not(is_odd))
    def _():
        for i in range(max(final - 1, 0), half):
            g_wait(i, base0 + i * tile, tile, i % 2)
    for i in range(final):
        g_copies(i, their_base + i * tile, tile, i % 2)[1].wait_recv()

    @pl.when(is_odd)
    def _():
        g_copies(final, their_base + final * tile, tile, final % 2)[1].wait_recv()

    @pl.when(jnp.logical_not(is_odd))
    def _():
        g_copies(final, tail_base, tail, final % 2)[1].wait_recv()
    for idx in range(6):
        out_copy(idx).wait()


def table_kernel(block, meta, loss_in, n_all, dx_all, g_ref, xa, ac, dy, dh, loss_o, out_ref, dw1_o, dw2_o, dx_wide, acts, dw, sems):
    i = pl.program_id(0)
    num_tok, dim = dx_all.shape
    loads = [pltpu.make_async_copy(src, acts.at[j], sems.at[j]) for j, src in enumerate((ac, dy, xa, dh))]
    stores = [pltpu.make_async_copy(dw.at[j], dst, sems.at[4 + j]) for j, dst in enumerate((dw2_o, dw1_o))]

    @pl.when(i == 0)
    def _():
        for load in loads:
            load.start()
        dx_wide[...] = dx_all[...].astype(F32)
        loss_o[0] = jnp.max(loss_in[...])

    out_ref[...] = dot_of(g_ref[...], n_all[...], 1, 0)

    def add(k, carry):
        row = meta[0, k] - i * block
        out_ref[pl.ds(row, 1), :] += dx_wide[pl.ds(meta[1, k], 1), :]
        return carry
    lax.fori_loop(meta[2, i], meta[2, i + 1], add, 0)

    for j in range(2):
        @pl.when(i == 1 + j)
        def _():
            loads[2 * j].wait()
            loads[2 * j + 1].wait()
            dw[j] = dot_of(acts[2 * j], acts[2 * j + 1], 0, 0)
            stores[j].start()

    @pl.when(i == pl.num_programs(0) - 1)
    def _():
        for store in stores:
            store.wait()


def solution(mesh):
    num_tp, num_pp = mesh.shape['tp'], mesh.shape['pp']

    def device_fn(tokens, labels, emb_table, w_in, w_out):
        num_micro, seq = tokens.shape
        vocab, dim = emb_table.shape
        cols = w_in.shape[2]
        num_tok = num_micro * seq
        chunk = row_chunk(vocab)
        chunks = vocab // chunk
        half = 6 if chunks >= 60 else 2
        tile = chunk * pl.cdiv(chunks, 2 * half)
        vmem, hbm = pl.BlockSpec(memory_space=pltpu.VMEM), pl.BlockSpec(memory_space=pl.ANY)
        act = (num_tp, seq, dim)
        wide = (num_tp, seq, cols)
        shape = jax.ShapeDtypeStruct
        dma = pltpu.SemaphoreType.DMA
        loss, meta, g_all, n_all, dx_all, x_all, a_cols, dy_all, dh_cols = pl.pallas_call(
            functools.partial(step_kernel, num_tp, num_pp, tile, half),
            out_shape=(shape((8, 128), F32), shape((8, num_tok), jnp.int32), shape((vocab, num_tok), BF16),
                       shape(act, BF16), shape(act, BF16), shape(act, BF16), shape(wide, BF16), shape(act, BF16), shape(wide, BF16)),
            in_specs=[vmem, vmem, hbm, hbm, hbm],
            out_specs=(vmem, vmem, hbm, hbm, hbm, hbm, hbm, hbm, hbm),
            scratch_shapes=[
                pltpu.VMEM(act, BF16), pltpu.VMEM(act, BF16), pltpu.VMEM((num_tp, dim, cols), BF16), pltpu.VMEM((num_tp, cols, dim), BF16),
                pltpu.VMEM((num_tp, cols, dim), BF16), pltpu.VMEM((num_tp, dim, cols), BF16),
                pltpu.VMEM((1, seq, dim), BF16), pltpu.VMEM((2, seq, dim), BF16), pltpu.VMEM(wide, BF16), pltpu.VMEM(wide, F32),
                pltpu.VMEM(act, BF16), pltpu.VMEM(act, BF16), pltpu.VMEM(wide, BF16), pltpu.VMEM(act, BF16), pltpu.VMEM(wide, BF16),
                pltpu.VMEM(wide, BF16), pltpu.VMEM((1, seq, dim), BF16), pltpu.VMEM(act, BF16),
                pltpu.VMEM((half * tile, num_tok), F32), pltpu.VMEM((2 * num_tp, 8, num_tok), F32),
                pltpu.VMEM(act, BF16), pltpu.VMEM(act, BF16), pltpu.VMEM(act, BF16),
                pltpu.VMEM((2, tile, num_tok), BF16), pltpu.VMEM((num_tok, 128), F32),
                dma((6,)), dma((6,)), dma((5,)), dma((5,)), dma((8, num_tp)), dma((8, num_tp)), dma((2, 3, num_tp)),
                dma((2 * num_tp,)), dma((2 * num_tp,)), dma((2,)), dma((half,)), dma((6,)), dma((6,)),
            ],
            compiler_params=pltpu.CompilerParams(collective_id=0, has_side_effects=True, vmem_limit_bytes=67043328),
            name='step_kernel',
        )(tokens.reshape(1, num_tok), labels.reshape(1, num_tok), emb_table, w_in[0], w_out[0])

        whole = lambda shp: pl.BlockSpec(shp, lambda i, meta: (0, 0))
        flat = lambda arr: arr.reshape(num_tok, arr.shape[2])
        loss, grad_table, grad_one, grad_two = pl.pallas_call(
            functools.partial(table_kernel, tile),
            grid_spec=pltpu.PrefetchScalarGridSpec(
                num_scalar_prefetch=1,
                grid=(pl.cdiv(vocab, tile),),
                in_specs=[whole((8, 128)), whole((num_tok, dim)), whole((num_tok, dim)), pl.BlockSpec((tile, num_tok), lambda i, meta: (i, 0)), hbm, hbm, hbm, hbm],
                out_specs=(pl.BlockSpec(memory_space=pltpu.SMEM), pl.BlockSpec((tile, dim), lambda i, meta: (i, 0)), hbm, hbm),
                scratch_shapes=[pltpu.VMEM((num_tok, dim), F32), pltpu.VMEM((4, num_tok, dim), BF16), pltpu.VMEM((2, dim, dim), F32), dma((6,))],
            ),
            out_shape=(shape((1,), F32), shape((vocab, dim), F32), shape((dim, cols), F32), shape((cols, dim), F32)),
            compiler_params=pltpu.CompilerParams(dimension_semantics=('arbitrary',), vmem_limit_bytes=67043328),
            name='table_kernel',
        )(meta, loss, flat(n_all), flat(dx_all), g_all, flat(x_all), flat(a_cols), flat(dy_all), flat(dh_cols))
        return loss, grad_one[None], grad_two[None], grad_table

    return jax.shard_map(device_fn, mesh=mesh, in_specs=(P('dp', None), P('dp', None), P('tp', None), P('pp', None, 'tp'), P('pp', 'tp', None)), out_specs=(P('dp'), P(('dp', 'pp'), None, 'tp'), P(('dp', 'pp'), 'tp', None), P(('dp', 'tp'), None)), check_vma=False)
```

```python
import functools

import jax
import jax.numpy as jnp
from jax import lax
from jax.experimental import pallas as pl
from jax.experimental.pallas import tpu as pltpu
from jax.sharding import PartitionSpec as P

NORM_EPS = 1e-6
MESH_ID = pl.DeviceIdType.MESH
GELU_C = 0.7978845608028654
GELU_A = 0.044715
BF16 = jnp.bfloat16
F32 = jnp.float32


def dot_of(lhs, rhs, lhs_dim, rhs_dim):
    return lax.dot_general(lhs, rhs, (((lhs_dim,), (rhs_dim,)), ((), ())), preferred_element_type=F32)


def row_chunk(rows):
    return max(size for size in range(16, 129, 16) if rows % size == 0)


def gelu_pair(hid):
    sq = hid * hid
    tanh = jnp.tanh(GELU_C * (hid + GELU_A * (hid * sq)))
    cdf = 0.5 * (1.0 + tanh)
    slope = cdf + (0.5 * GELU_C) * hid * (1.0 - tanh * tanh) * (1.0 + (3.0 * GELU_A) * sq)
    return hid * cdf, slope


def step_kernel(num_tp, num_pp, tile, half, tok, lab, e_hbm, w1_hbm, w2_hbm,
                loss_o, meta_o, g_o, n_o, dx_o, xa_o, ac_o, dy_o, dh_o,
                x0, x0r, w1s, w2s, w1t, w2t, x_in, y_buf, a_own, slope, n_all, x_all, a_cols, dy_all, dh_cols, dh_own, dy_in, dx_all,
                logit, stat, dn_send, dn_recv, dn_half, g_buf, key_buf, via_x, via_y,
                w_send, w_recv, p_send, p_recv, tp_send, tp_recv, tree_send, st_send, st_recv, g_send, g_recv, out_sem, loc, via_send, via_recv):
    rank = lax.axis_index('tp')
    stage = lax.axis_index('pp')
    last = num_pp - 1
    is_first = stage == 0
    is_last = stage == last
    _, seq, dim = x_in.shape
    vocab = e_hbm.shape[0]
    chunk = row_chunk(vocab)
    right = lax.rem(rank + 1, num_tp)
    left = lax.rem(rank + num_tp - 1, num_tp)
    opp = lax.rem(rank + 2, num_tp)
    X0, N, XA, AC, DY, DH, DX, DN = range(8)

    def push(src, dst, ssem, rsem, dev):
        return pltpu.make_async_remote_copy(src_ref=src, dst_ref=dst, send_sem=ssem, recv_sem=rsem, device_id=dev, device_id_type=MESH_ID)

    def swap(kind, src_of, dst, mode):
        for k in range(1, num_tp):
            peer = lax.rem(rank + k, num_tp)
            if mode == 'recv':
                push(dst.at[peer], dst.at[peer], tp_send.at[kind, k], tp_recv.at[kind, peer], {'tp': rank}).wait_recv()
            else:
                copy = push(src_of(peer), dst.at[rank], tp_send.at[kind, k], tp_recv.at[kind, rank], {'tp': peer})
                copy.start() if mode == 'start' else copy.wait_send()

    num_x = num_pp // 2
    chip, core = stage // 2, lax.rem(stage, 2)
    partner = chip * 2 + 1 - core
    is_top = chip == num_x - 1
    is_lookup = stage == last - 1
    mirror = (num_x - 1 - chip) * 2 + core

    def tree(kind, tid, buf, root, mode):
        root_x, root_c = root // 2, root % 2
        on_core = core == root_c
        plus = lax.rem(chip + 1, num_x) * 2 + root_c
        minus = lax.rem(chip + num_x - 1, num_x) * 2 + root_c
        at_root = jnp.logical_and(on_core, chip == root_x)
        at_next = jnp.logical_and(on_core, jnp.logical_or(chip == root_x, chip == (root_x + 1) % num_x))
        for i in range(num_tp):
            blk = lax.rem(rank + i, num_tp)

            def go(slot, dest):
                copy = push(buf.at[blk], buf.at[blk], tree_send.at[tid, slot, i], tp_recv.at[kind, blk], {'pp': dest})
                copy.start() if mode == 'start' else copy.wait_send()

            if mode == 'start':
                wait = push(buf.at[blk], buf.at[blk], tree_send.at[tid, 0, i], tp_recv.at[kind, blk], {'pp': stage})
                if i == 0:
                    pl.when(stage != root)(wait.wait_recv)
                else:
                    wait.wait_recv()

            @pl.when(on_core)
            def _():
                go(2, partner)

            @pl.when(at_root)
            def _():
                go(0, minus)

            @pl.when(at_next)
            def _():
                go(1, plus)

    barrier = pltpu.get_barrier_semaphore()
    for k in range(1, num_tp):
        for pp in (stage, partner):
            pl.semaphore_signal(barrier, inc=1, device_id={'tp': lax.rem(rank + k, num_tp), 'pp': pp}, device_id_type=MESH_ID)
    for k in range(1, num_pp):
        pl.semaphore_signal(barrier, inc=1, device_id={'pp': lax.rem(stage + k, num_pp)}, device_id_type=MESH_ID)
    pl.semaphore_wait(barrier, 2 * (num_tp - 1) + num_pp - 1)

    own1 = pltpu.make_async_copy(w1_hbm, w1s.at[rank], loc.at[0])
    own2 = pltpu.make_async_copy(w2_hbm, w2s.at[rank], loc.at[1])
    own1.start()
    own2.start()

    rows_w = w1_hbm.shape[0]
    detours = [(0, rows_w // 2), (1, rows_w // 4)] if num_x >= 4 else []

    def w_copy(idx, rows=None):
        src, full, who, dev = [
            (w1_hbm, w1s, rank, right), (w2_hbm, w2s, rank, right), (w1_hbm, w1s, rank, left), (w2_hbm, w2s, rank, left),
            (w1s.at[left], w1s, left, right), (w2s.at[right], w2s, right, left)][idx]
        if rows is None:
            return push(src, full.at[who], w_send.at[idx], w_recv.at[idx], {'tp': dev})
        part = pl.ds(0, rows)
        return push(src.at[part], full.at[who, part], w_send.at[idx], w_recv.at[idx], {'tp': dev})

    def w_wait(idx, rows=None):
        full, who = [(w1s, left), (w2s, left), (w1s, right), (w2s, right), (w1s, opp), (w2s, opp)][idx]
        view = full.at[who] if rows is None else full.at[who, pl.ds(0, rows)]
        push(view, view, w_send.at[idx], w_recv.at[idx], {'tp': rank}).wait_recv()

    def by_chip(action):
        for near, size in detours:
            pl.when(chip == near)(functools.partial(action, rows_w - size))
        pl.when(chip >= len(detours))(functools.partial(action, None))

    def detour(size, leg, j):
        part = pl.ds(0, size)
        tail_rows = pl.ds(rows_w - size, size)
        if leg == 0:
            src = (w2_hbm, w1_hbm)[j].at[tail_rows]
            return push(src, via_x.at[j, part], via_send.at[j], via_recv.at[j], {'pp': mirror})
        if leg == 1:
            return push(via_x.at[j, part], via_y.at[j, part], via_send.at[2 + j], via_recv.at[2 + j], {'tp': (right, left)[j]})
        full, who = ((w2s, left), (w1s, right))[j]
        return push(via_y.at[j, part], full.at[who, tail_rows], via_send.at[4 + j], via_recv.at[4 + j], {'pp': mirror})

    def on_detour(helper, action):
        for near, size in detours:
            pl.when(chip == (num_x - 1 - near if helper else near))(functools.partial(action, size))

    w_copy(0).start()
    w_copy(3).start()

    def leave(size):
        for j in range(2):
            detour(size, 0, j).start()

    def pass_on(size):
        for j in range(2):
            detour(size, 0, j).wait_recv()
            detour(size, 1, j).start()

    def bring_back(size):
        for j in range(2):
            detour(size, 1, j).wait_recv()
            detour(size, 2, j).start()

    def arrive(size):
        for j in range(2):
            detour(size, 2, j).wait_recv()

    def second(rows):
        w_copy(1, rows).start()
        w_copy(2, rows).start()

    on_detour(False, leave)
    on_detour(True, pass_on)

    @pl.when(jnp.logical_not(is_lookup))
    def _():
        by_chip(second)

    def flip(src, dst, who):
        def one(j, carry):
            part = pl.ds(pl.multiple_of(j * 128, 128), 128)
            dst[who, :, part] = jnp.transpose(src[who, part, :])
            return carry
        lax.fori_loop(0, src.shape[1] // 128, one, 0)

    num_tok = num_tp * seq
    vocab_base = rank * vocab
    tail_base = (2 * half - 1) * tile
    tail = vocab - tail_base
    tok_row = tok[...] - vocab_base
    lab_row = lab[...] - vocab_base
    rows_in = lax.broadcasted_iota(jnp.int32, (chunk // 8, 8, num_tok), 0) * 8 + lax.broadcasted_iota(jnp.int32, (chunk // 8, 8, num_tok), 1)

    def at(i):
        return pl.multiple_of(i * tile, 16)

    def fetch(e_buf, base, size, slot):
        return pltpu.make_async_copy(e_hbm.at[pl.ds(base, size)], e_buf.at[slot, pl.ds(0, size)], loc.at[2 + slot])

    def sort_tokens():
        key_row = jnp.where(jnp.logical_and(tok_row >= 0, tok_row < vocab), tok_row, 1 << 20).astype(F32)
        lanes = lax.broadcasted_iota(jnp.int32, (1, num_tok), 1).astype(F32)
        step = 128
        key_buf[...] = jnp.transpose(jnp.broadcast_to(key_row, (step, num_tok)))

        def count(b, pos):
            here = key_buf[pl.ds(pl.multiple_of(b * step, step), step), 0:1]
            idx = (lax.broadcasted_iota(jnp.int32, (step, 1), 0) + b * step).astype(F32)
            ahead = jnp.logical_or(here < key_row, jnp.logical_and(here == key_row, idx < lanes))
            return pos + jnp.sum(jnp.where(ahead, 1.0, 0.0), axis=0, keepdims=True)

        def starts(b, acc):
            here = key_buf[pl.ds(pl.multiple_of(b * step, step), step), 0:1]
            return acc + jnp.sum(jnp.where(here < lanes * tile, 1.0, 0.0), axis=0, keepdims=True)

        zero = jnp.zeros((1, num_tok), F32)
        pos_row = lax.fori_loop(0, num_tok // step, count, zero)
        offs = lax.fori_loop(0, num_tok // step, starts, zero)

        def place(b, carry):
            keys, idxs = carry
            here = key_buf[pl.ds(pl.multiple_of(b * step, step), step), 0:1]
            pos = key_buf[pl.ds(pl.multiple_of(b * step, step), step), 1:2]
            idx = (lax.broadcasted_iota(jnp.int32, (step, 1), 0) + b * step).astype(F32)
            mine = pos == lanes
            keys = keys + jnp.sum(jnp.where(mine, here, 0.0), axis=0, keepdims=True)
            return keys, idxs + jnp.sum(jnp.where(mine, idx, 0.0), axis=0, keepdims=True)

        both = jnp.where(lax.broadcasted_iota(jnp.int32, (step, num_tok), 0) == 0, key_row, pos_row)
        key_buf[...] = jnp.transpose(both)
        keys, idxs = lax.fori_loop(0, num_tok // step, place, (zero, zero))
        line = lax.broadcasted_iota(jnp.int32, (8, num_tok), 0)
        meta_o[...] = jnp.where(line == 0, keys, jnp.where(line == 1, idxs, offs)).astype(jnp.int32)

    sort_tokens()

    def lookup_pass(e_buf, acc):
        def tile_of(base, size, slot):
            def one(c, carry):
                row = base + c * chunk
                hot = jnp.where(rows_in == (tok_row - row)[None], 1.0, 0.0)
                g_buf[slot, pl.ds(pl.multiple_of(c * chunk, chunk), chunk), :] = hot.reshape(chunk, num_tok).astype(BF16)
                return carry
            lax.fori_loop(0, size // chunk, one, 0)
            fetch(e_buf, base, size, slot).wait()
            acc[...] += dot_of(g_buf[slot, pl.ds(0, size), :], e_buf[slot, pl.ds(0, size), :], 0, 0)

        acc[...] = jnp.zeros_like(acc)
        fetch(e_buf, 0, tile, 0).start()
        count = 2 * half - 1

        def one(i, carry):
            slot = lax.rem(i, 2)

            @pl.when(i + 1 < count)
            def _():
                fetch(e_buf, at(i + 1), tile, 1 - slot).start()
            tile_of(at(i), tile, slot)
            return carry
        lax.fori_loop(0, count, one, 0)
        fetch(e_buf, tail_base, tail, 0).start()
        tile_of(tail_base, tail, 0)
        for k in range(num_tp):
            x0[k] = acc[k * seq:(k + 1) * seq, :].astype(BF16)

    @pl.when(is_lookup)
    def _():
        pl.run_scoped(lookup_pass, pltpu.VMEM((2, tile, dim), BF16), pltpu.VMEM((num_tok, dim), F32))
        swap(X0, lambda peer: x0.at[peer], x0r, 'start')
        second(None)

    on_detour(True, bring_back)
    first_x = push(y_buf.at[pl.ds(1, 1)], x_in, p_send.at[5], p_recv.at[5], {'pp': 0})

    @pl.when(is_lookup)
    def _():
        swap(X0, None, x0r, 'recv')
        total = x0[rank].astype(F32)
        for k in range(1, num_tp):
            total = total + x0r[lax.rem(rank + k, num_tp)].astype(F32)
        y_buf[1] = total.astype(BF16)
        first_x.start()

    own1.wait()
    own2.wait()
    flip(w1s, w1t, rank)
    flip(w2s, w2t, rank)
    w_wait(0)
    w_copy(4).start()
    w_wait(3)
    w_copy(5).start()
    flip(w1s, w1t, left)
    flip(w2s, w2t, right)

    @pl.when(is_lookup)
    def _():
        first_x.wait_send()

    def second_in(rows):
        w_wait(1, rows)
        w_wait(2, rows)

    by_chip(second_in)
    on_detour(False, arrive)
    flip(w2s, w2t, left)
    flip(w1s, w1t, right)
    w_wait(4)
    w_wait(5)

    cols = w1s.shape[2]
    piece = 256 if cols % 256 == 0 and dim % 256 == 0 else 128
    cut = dim // 3 // 128 * 128
    spans = [(0, cut), (cut, dim - cut)] if cut else [(0, dim)]

    def hop(kind, src, dst, part, dest):
        lo, size = spans[part]
        view = (0, slice(None), pl.ds(lo, size))
        return push(src.at[view], dst.at[view], p_send.at[2 * kind + part], p_recv.at[2 * kind + part], {'pp': dest})

    def hops(kind, mode):
        src, dst = (y_buf.at[pl.ds(0, 1)], x_in) if kind == 0 else (y_buf.at[pl.ds(1, 1)], dy_in)
        dest = jnp.minimum(stage + 1, last) if kind == 0 else jnp.maximum(stage - 1, 0)
        return [hop(kind, src, dst, part, dest) for part in range(len(spans))]

    def send_rows(kind, source, acts, mats, active):
        for part, (lo, size) in enumerate(spans):
            for off in range(lo, lo + size, piece):
                total = source[0, :, off:off + piece].astype(F32)
                for blk in range(num_tp):
                    total = total + dot_of(acts[blk], mats[blk, :, off:off + piece], 1, 0)
                y_buf[kind, :, off:off + piece] = total.astype(BF16)

            @pl.when(active)
            def _():
                hops(kind, 'start')[part].start()

    @pl.when(jnp.logical_not(is_first))
    def _():
        for copy in hops(0, 'recv'):
            copy.wait_recv()

    @pl.when(is_first)
    def _():
        first_x.wait_recv()

    x_act = x_in[0]
    for blk in range(num_tp):
        for off in range(0, cols, piece):
            gate, grad = gelu_pair(dot_of(x_act, w1s[blk, :, off:off + piece], 1, 0))
            a_own[blk, :, off:off + piece] = gate.astype(BF16)
            slope[blk, :, off:off + piece] = grad
    send_rows(0, x_in, a_own, w2s, jnp.logical_not(is_last))

    def norm_of():
        wide = y_buf[0].astype(F32)
        inv_rms = lax.rsqrt(jnp.mean(wide * wide, axis=-1, keepdims=True) + NORM_EPS)
        return inv_rms, wide * inv_rms

    @pl.when(is_last)
    def _():
        n_all[rank] = norm_of()[1].astype(BF16)
        swap(N, lambda peer: n_all.at[rank], n_all, 'start')

    flip(w1s, w1t, opp)
    flip(w2s, w2t, opp)
    tree(N, 0, n_all, last, 'start')
    x_all[rank] = x_in[0]
    a_cols[rank] = a_own[rank]
    swap(XA, lambda peer: x_in.at[0], x_all, 'start')
    swap(AC, lambda peer: a_own.at[peer], a_cols, 'start')
    outs = [(n_all, n_o), (dx_all, dx_o), (x_all, xa_o), (a_cols, ac_o), (dy_all, dy_o), (dh_cols, dh_o)]

    def out_copy(idx):
        return pltpu.make_async_copy(outs[idx][0], outs[idx][1], out_sem.at[idx])

    out_copy(0).start()
    normed = n_all[...].reshape(num_tok, dim)
    base0 = core * (half * tile)
    mine = half - core
    is_odd = core == 1

    def stats_of(base, count, carry):
        def one(c, carry):
            top, acc, hit = carry
            row = pl.multiple_of(base + c * chunk, chunk)
            part = logit[pl.ds(row, chunk), :].reshape(chunk // 8, 8, num_tok)
            new = jnp.maximum(top, jnp.max(part, axis=0))
            acc = acc * jnp.exp(top - new) + jnp.sum(jnp.exp(part - new[None]), axis=0)
            hit = hit + jnp.sum(jnp.where(rows_in == (lab_row - (base0 + row))[None], part, 0.0), axis=0)
            return new, acc, hit
        return lax.fori_loop(0, count // chunk, one, carry)

    slot_of = rank * 2 + core

    def logits_pass(e_buf):
        def finish(carry):
            top, acc, hit = carry
            peak = jnp.max(top, axis=0, keepdims=True)
            total = jnp.sum(acc * jnp.exp(top - peak), axis=0, keepdims=True)
            hits = jnp.sum(hit, axis=0, keepdims=True)
            line = lax.broadcasted_iota(jnp.int32, (8, num_tok), 0)
            stat[slot_of] = jnp.where(line == 0, peak, jnp.where(line == 1, total, hits))

        def one(i, carry):
            slot = lax.rem(i, 2)

            @pl.when(i + 1 < mine)
            def _():
                fetch(e_buf, base0 + at(i + 1), tile, 1 - slot).start()
            fetch(e_buf, base0 + at(i), tile, slot).wait()
            logit[pl.ds(at(i), tile), :] = dot_of(e_buf[slot], normed, 1, 1)
            return stats_of(at(i), tile, carry)

        zero = jnp.zeros((8, num_tok), F32)
        fetch(e_buf, base0, tile, 0).start()
        carry = lax.fori_loop(0, mine, one, (jnp.full((8, num_tok), -jnp.inf, F32), zero, zero))

        @pl.when(is_odd)
        def _():
            slot = (half - 1) % 2
            fetch(e_buf, tail_base, tail, slot).start()
            fetch(e_buf, tail_base, tail, slot).wait()
            logit[pl.ds((half - 1) * tile, tail), :] = dot_of(e_buf[slot, pl.ds(0, tail), :], normed, 1, 1)
            finish(stats_of((half - 1) * tile, tail, carry))

        @pl.when(jnp.logical_not(is_odd))
        def _():
            finish(carry)

    pl.run_scoped(logits_pass, pltpu.VMEM((2, tile, dim), BF16))

    def stats_swap(mode):
        for k in range(num_tp):
            for flip in range(2):
                if k == 0 and flip == 0:
                    continue
                peer = lax.rem(rank + k, num_tp)
                peer_core = core if flip == 0 else 1 - core
                theirs = peer * 2 + peer_core
                if mode == 'recv':
                    push(stat.at[theirs], stat.at[theirs], st_send.at[2 * k + flip], st_recv.at[theirs], {'tp': rank}).wait_recv()
                else:
                    copy = push(stat.at[slot_of], stat.at[slot_of], st_send.at[2 * k + flip], st_recv.at[slot_of],
                                {'tp': peer, 'pp': chip * 2 + peer_core})
                    copy.start() if mode == 'start' else copy.wait_send()

    stats_swap('start')
    stats_swap('recv')
    peak = stat[0, 0:1, :]
    for j in range(1, 2 * num_tp):
        peak = jnp.maximum(peak, stat[j, 0:1, :])
    total = jnp.zeros_like(peak)
    target = jnp.zeros_like(peak)
    for j in range(2 * num_tp):
        total = total + stat[j, 1:2, :] * jnp.exp(stat[j, 0:1, :] - peak)
        target = target + stat[j, 2:3, :]
    log_norm = peak + jnp.log(total)
    loss = jnp.sum(log_norm - target, axis=1, keepdims=True) / num_tok
    loss_o[...] = jnp.broadcast_to(loss, loss_o.shape)
    norm_rows = jnp.broadcast_to(log_norm, (8, num_tok))

    def grad_tile(base, count, slot):
        def one(c, carry):
            row = pl.multiple_of(base + c * chunk, chunk)
            part = logit[pl.ds(row, chunk), :].reshape(chunk // 8, 8, num_tok)
            hit = jnp.where(rows_in == (lab_row - (base0 + row))[None], 1.0, 0.0)
            part = jnp.exp(part - norm_rows[None]) - hit
            g_buf[slot, pl.ds(pl.multiple_of(c * chunk, chunk), chunk), :] = part.reshape(chunk, num_tok).astype(BF16)
            return carry
        lax.fori_loop(0, count // chunk, one, 0)

    def g_copies(i, base, size, slot):
        here, there = g_buf.at[slot, pl.ds(0, size)], g_o.at[pl.ds(base, size)]
        return pltpu.make_async_copy(here, there, loc.at[4 + slot]), push(here, there, g_send.at[slot], g_recv.at[i], {'pp': partner})

    def g_start(i, base, size, slot):
        for copy in g_copies(i, base, size, slot):
            copy.start()

    def g_wait(i, base, size, slot):
        keep, send = g_copies(i, base, size, slot)
        keep.wait()
        send.wait_send()

    def grads_pass(e_buf, dn_acc):
        @pl.when(is_top)
        def _():
            dn_acc[...] = jnp.zeros_like(dn_acc)
            fetch(e_buf, base0, tile, 0).start()

        def one(i, carry):
            slot = lax.rem(i, 2)

            @pl.when(i >= 2)
            def _():
                g_wait(i - 2, base0 + at(i - 2), tile, slot)
            grad_tile(at(i), tile, slot)
            g_start(i, base0 + at(i), tile, slot)

            @pl.when(is_top)
            def _():
                @pl.when(i + 1 < mine)
                def _():
                    fetch(e_buf, base0 + at(i + 1), tile, 1 - slot).start()
                fetch(e_buf, base0 + at(i), tile, slot).wait()
                dn_acc[...] += dot_of(g_buf[slot], e_buf[slot], 0, 0)
            return carry

        lax.fori_loop(0, mine, one, 0)
        final = half - 1
        slot = final % 2

        @pl.when(is_odd)
        def _():
            @pl.when(is_top)
            def _():
                fetch(e_buf, tail_base, tail, slot).start()
            if final >= 2:
                g_wait(final - 2, base0 + (final - 2) * tile, tile, slot)
            grad_tile(final * tile, tail, slot)
            g_start(final, tail_base, tail, slot)

            @pl.when(is_top)
            def _():
                fetch(e_buf, tail_base, tail, slot).wait()
                dn_acc[...] += dot_of(g_buf[slot, pl.ds(0, tail), :], e_buf[slot, pl.ds(0, tail), :], 0, 0)
        to_top = push(dn_send, dn_half, p_send.at[4], p_recv.at[4], {'pp': partner})

        @pl.when(jnp.logical_and(is_top, jnp.logical_not(is_last)))
        def _():
            for k in range(num_tp):
                dn_send[k] = dn_acc[k * seq:(k + 1) * seq, :].astype(BF16)
            to_top.start()

        @pl.when(is_last)
        def _():
            to_top.wait_recv()
            for k in range(num_tp):
                both = dn_acc[k * seq:(k + 1) * seq, :] + dn_half[k].astype(F32)
                dn_acc[k * seq:(k + 1) * seq, :] = both
                dn_send[k] = both.astype(BF16)
            swap(DN, lambda peer: dn_send.at[peer], dn_recv, 'start')
            swap(DN, None, dn_recv, 'recv')
            grad_n = dn_acc[pl.ds(pl.multiple_of(rank * seq, seq), seq), :]
            for k in range(1, num_tp):
                grad_n = grad_n + dn_recv[lax.rem(rank + k, num_tp)].astype(F32)
            inv_rms, unit = norm_of()
            dy_in[0] = (inv_rms * (grad_n - unit * jnp.mean(unit * grad_n, axis=-1, keepdims=True))).astype(BF16)

    pl.run_scoped(grads_pass, pltpu.VMEM((2, tile, dim), BF16), pltpu.VMEM((num_tok, dim), F32))

    @pl.when(jnp.logical_not(is_last))
    def _():
        for copy in hops(1, 'recv'):
            copy.wait_recv()

    dy_all[rank] = dy_in[0]
    swap(DY, lambda peer: dy_in.at[0], dy_all, 'start')
    grad_y = dy_in[0]
    for blk in range(num_tp):
        for off in range(0, cols, piece):
            grad_a = dot_of(grad_y, w2t[blk, :, off:off + piece], 1, 0)
            dh_own[blk, :, off:off + piece] = (slope[blk, :, off:off + piece] * grad_a).astype(BF16)
    send_rows(1, dy_in, dh_own, w1t, jnp.logical_not(is_first))

    @pl.when(is_first)
    def _():
        dx_all[rank] = y_buf[1]
        swap(DX, lambda peer: y_buf.at[1], dx_all, 'start')

    dh_cols[rank] = dh_own[rank]

    @pl.when(chip != 0)
    def _():
        swap(DH, lambda peer: dh_own.at[peer], dh_cols, 'start')

    tree(DX, 1, dx_all, 0, 'start')

    @pl.when(chip == 0)
    def _():
        swap(DH, lambda peer: dh_own.at[peer], dh_cols, 'start')

    out_copy(1).start()
    for idx, kind, dst in ((2, XA, x_all), (3, AC, a_cols), (4, DY, dy_all), (5, DH, dh_cols)):
        swap(kind, None, dst, 'recv')
        out_copy(idx).start()

    for idx in (0, 3, 4, 5):
        w_copy(idx).wait_send()

    def second_sent(rows):
        w_copy(1, rows).wait_send()
        w_copy(2, rows).wait_send()

    def left_sent(size):
        for j in range(2):
            detour(size, 0, j).wait_send()

    def help_sent(size):
        for j in range(2):
            detour(size, 1, j).wait_send()
            detour(size, 2, j).wait_send()

    by_chip(second_sent)
    on_detour(False, left_sent)
    on_detour(True, help_sent)

    @pl.when(is_lookup)
    def _():
        swap(X0, lambda peer: x0.at[peer], x0r, 'sent')

    @pl.when(is_first)
    def _():
        swap(DX, lambda peer: y_buf.at[1], dx_all, 'sent')

    @pl.when(is_last)
    def _():
        swap(N, lambda peer: n_all.at[rank], n_all, 'sent')
        swap(DN, lambda peer: dn_send.at[peer], dn_recv, 'sent')

    @pl.when(jnp.logical_and(is_top, jnp.logical_not(is_last)))
    def _():
        push(dn_send, dn_half, p_send.at[4], p_recv.at[4], {'pp': partner}).wait_send()

    @pl.when(jnp.logical_not(is_last))
    def _():
        for copy in hops(0, 'sent'):
            copy.wait_send()

    @pl.when(jnp.logical_not(is_first))
    def _():
        for copy in hops(1, 'sent'):
            copy.wait_send()
    swap(XA, lambda peer: x_in.at[0], x_all, 'sent')
    swap(AC, lambda peer: a_own.at[peer], a_cols, 'sent')
    swap(DY, lambda peer: dy_in.at[0], dy_all, 'sent')
    swap(DH, lambda peer: dh_own.at[peer], dh_cols, 'sent')
    stats_swap('sent')
    tree(N, 0, n_all, last, 'sent')
    tree(DX, 1, dx_all, 0, 'sent')

    final = half - 1
    their_base = (1 - core) * (half * tile)

    @pl.when(is_odd)
    def _():
        if final >= 1:
            g_wait(final - 1, base0 + (final - 1) * tile, tile, (final - 1) % 2)
        g_wait(final, tail_base, tail, final % 2)

    @pl.when(jnp.logical_not(is_odd))
    def _():
        for i in range(max(final - 1, 0), half):
            g_wait(i, base0 + i * tile, tile, i % 2)
    for i in range(final):
        g_copies(i, their_base + i * tile, tile, i % 2)[1].wait_recv()

    @pl.when(is_odd)
    def _():
        g_copies(final, their_base + final * tile, tile, final % 2)[1].wait_recv()

    @pl.when(jnp.logical_not(is_odd))
    def _():
        g_copies(final, tail_base, tail, final % 2)[1].wait_recv()
    for idx in range(6):
        out_copy(idx).wait()


def table_kernel(block, meta, loss_in, n_all, dx_all, g_ref, xa, ac, dy, dh, loss_o, out_ref, dw1_o, dw2_o, dx_wide, acts, dw, sems):
    i = pl.program_id(0)
    num_tok, dim = dx_all.shape
    loads = [pltpu.make_async_copy(src, acts.at[j], sems.at[j]) for j, src in enumerate((ac, dy, xa, dh))]
    stores = [pltpu.make_async_copy(dw.at[j], dst, sems.at[4 + j]) for j, dst in enumerate((dw2_o, dw1_o))]

    @pl.when(i == 0)
    def _():
        for load in loads:
            load.start()
        dx_wide[...] = dx_all[...].astype(F32)
        loss_o[0] = jnp.max(loss_in[...])

    out_ref[...] = dot_of(g_ref[...], n_all[...], 1, 0)

    def add(k, carry):
        row = meta[0, k] - i * block
        out_ref[pl.ds(row, 1), :] += dx_wide[pl.ds(meta[1, k], 1), :]
        return carry
    lax.fori_loop(meta[2, i], meta[2, i + 1], add, 0)

    for j in range(2):
        @pl.when(i == 1 + j)
        def _():
            loads[2 * j].wait()
            loads[2 * j + 1].wait()
            dw[j] = dot_of(acts[2 * j], acts[2 * j + 1], 0, 0)
            stores[j].start()

    @pl.when(i == pl.num_programs(0) - 1)
    def _():
        for store in stores:
            store.wait()


def solution(mesh):
    num_tp, num_pp = mesh.shape['tp'], mesh.shape['pp']

    def device_fn(tokens, labels, emb_table, w_in, w_out):
        num_micro, seq = tokens.shape
        vocab, dim = emb_table.shape
        cols = w_in.shape[2]
        num_tok = num_micro * seq
        chunk = row_chunk(vocab)
        chunks = vocab // chunk
        half = 6 if chunks >= 60 else 2
        tile = chunk * pl.cdiv(chunks, 2 * half)
        vmem, hbm = pl.BlockSpec(memory_space=pltpu.VMEM), pl.BlockSpec(memory_space=pl.ANY)
        act = (num_tp, seq, dim)
        wide = (num_tp, seq, cols)
        shape = jax.ShapeDtypeStruct
        dma = pltpu.SemaphoreType.DMA
        loss, meta, g_all, n_all, dx_all, x_all, a_cols, dy_all, dh_cols = pl.pallas_call(
            functools.partial(step_kernel, num_tp, num_pp, tile, half),
            out_shape=(shape((8, 128), F32), shape((8, num_tok), jnp.int32), shape((vocab, num_tok), BF16),
                       shape(act, BF16), shape(act, BF16), shape(act, BF16), shape(wide, BF16), shape(act, BF16), shape(wide, BF16)),
            in_specs=[vmem, vmem, hbm, hbm, hbm],
            out_specs=(vmem, vmem, hbm, hbm, hbm, hbm, hbm, hbm, hbm),
            scratch_shapes=[
                pltpu.VMEM(act, BF16), pltpu.VMEM(act, BF16), pltpu.VMEM((num_tp, dim, cols), BF16), pltpu.VMEM((num_tp, cols, dim), BF16),
                pltpu.VMEM((num_tp, cols, dim), BF16), pltpu.VMEM((num_tp, dim, cols), BF16),
                pltpu.VMEM((1, seq, dim), BF16), pltpu.VMEM((2, seq, dim), BF16), pltpu.VMEM(wide, BF16), pltpu.VMEM(wide, F32),
                pltpu.VMEM(act, BF16), pltpu.VMEM(act, BF16), pltpu.VMEM(wide, BF16), pltpu.VMEM(act, BF16), pltpu.VMEM(wide, BF16),
                pltpu.VMEM(wide, BF16), pltpu.VMEM((1, seq, dim), BF16), pltpu.VMEM(act, BF16),
                pltpu.VMEM((half * tile, num_tok), F32), pltpu.VMEM((2 * num_tp, 8, num_tok), F32),
                pltpu.VMEM(act, BF16), pltpu.VMEM(act, BF16), pltpu.VMEM(act, BF16),
                pltpu.VMEM((2, tile, num_tok), BF16), pltpu.VMEM((num_tok, 128), F32),
                pltpu.VMEM((2, dim // 2, dim), BF16), pltpu.VMEM((2, dim // 2, dim), BF16),
                dma((6,)), dma((6,)), dma((6,)), dma((6,)), dma((8, num_tp)), dma((8, num_tp)), dma((2, 3, num_tp)),
                dma((2 * num_tp,)), dma((2 * num_tp,)), dma((2,)), dma((half,)), dma((6,)), dma((6,)), dma((6,)), dma((6,)),
            ],
            compiler_params=pltpu.CompilerParams(collective_id=0, has_side_effects=True, vmem_limit_bytes=67043328),
            name='step_kernel',
        )(tokens.reshape(1, num_tok), labels.reshape(1, num_tok), emb_table, w_in[0], w_out[0])

        whole = lambda shp: pl.BlockSpec(shp, lambda i, meta: (0, 0))
        flat = lambda arr: arr.reshape(num_tok, arr.shape[2])
        loss, grad_table, grad_one, grad_two = pl.pallas_call(
            functools.partial(table_kernel, tile),
            grid_spec=pltpu.PrefetchScalarGridSpec(
                num_scalar_prefetch=1,
                grid=(pl.cdiv(vocab, tile),),
                in_specs=[whole((8, 128)), whole((num_tok, dim)), whole((num_tok, dim)), pl.BlockSpec((tile, num_tok), lambda i, meta: (i, 0)), hbm, hbm, hbm, hbm],
                out_specs=(pl.BlockSpec(memory_space=pltpu.SMEM), pl.BlockSpec((tile, dim), lambda i, meta: (i, 0)), hbm, hbm),
                scratch_shapes=[pltpu.VMEM((num_tok, dim), F32), pltpu.VMEM((4, num_tok, dim), BF16), pltpu.VMEM((2, dim, dim), F32), dma((6,))],
            ),
            out_shape=(shape((1,), F32), shape((vocab, dim), F32), shape((dim, cols), F32), shape((cols, dim), F32)),
            compiler_params=pltpu.CompilerParams(dimension_semantics=('arbitrary',), vmem_limit_bytes=67043328),
            name='table_kernel',
        )(meta, loss, flat(n_all), flat(dx_all), g_all, flat(x_all), flat(a_cols), flat(dy_all), flat(dh_cols))
        return loss, grad_one[None], grad_two[None], grad_table

    return jax.shard_map(device_fn, mesh=mesh, in_specs=(P('dp', None), P('dp', None), P('tp', None), P('pp', None, 'tp'), P('pp', 'tp', None)), out_specs=(P('dp'), P(('dp', 'pp'), None, 'tp'), P(('dp', 'pp'), 'tp', None), P(('dp', 'tp'), None)), check_vma=False)
```

```python
import functools

import jax
import jax.numpy as jnp
from jax import lax
from jax.experimental import pallas as pl
from jax.experimental.pallas import tpu as pltpu
from jax.sharding import PartitionSpec as P

NORM_EPS = 1e-6
MESH_ID = pl.DeviceIdType.MESH
GELU_C = 0.7978845608028654
GELU_A = 0.044715
BF16 = jnp.bfloat16
F32 = jnp.float32


def dot_of(lhs, rhs, lhs_dim, rhs_dim):
    return lax.dot_general(lhs, rhs, (((lhs_dim,), (rhs_dim,)), ((), ())), preferred_element_type=F32)


def row_chunk(rows):
    return max(size for size in range(16, 129, 16) if rows % size == 0)


def gelu_pair(hid):
    sq = hid * hid
    tanh = jnp.tanh(GELU_C * (hid + GELU_A * (hid * sq)))
    cdf = 0.5 * (1.0 + tanh)
    slope = cdf + (0.5 * GELU_C) * hid * (1.0 - tanh * tanh) * (1.0 + (3.0 * GELU_A) * sq)
    return hid * cdf, slope


def step_kernel(num_tp, num_pp, tile, half, block, tok, lab, e_hbm, w1_hbm, w2_hbm,
                loss_o, meta_o, g_o, n_o, dx_o, xa_o, ac_o, dy_o, dh_o,
                x0, x0r, w1s, w2s, w1t, w2t, x_in, y_buf, a_own, slope, n_all, x_all, a_cols, dy_all, dh_cols, dh_own, dy_in, dx_all,
                logit, stat, dn_send, dn_recv, dn_half, g_buf, key_buf, via_x, via_y,
                w_send, w_recv, p_send, p_recv, tp_send, tp_recv, tree_send, st_send, st_recv, g_send, g_recv, out_sem, loc, via_send, via_recv):
    rank = lax.axis_index('tp')
    stage = lax.axis_index('pp')
    last = num_pp - 1
    is_first = stage == 0
    is_last = stage == last
    _, seq, dim = x_in.shape
    vocab = e_hbm.shape[0]
    chunk = row_chunk(vocab)
    right = lax.rem(rank + 1, num_tp)
    left = lax.rem(rank + num_tp - 1, num_tp)
    opp = lax.rem(rank + 2, num_tp)
    X0, N, XA, AC, DY, DH, DX, DN = range(8)

    def push(src, dst, ssem, rsem, dev):
        return pltpu.make_async_remote_copy(src_ref=src, dst_ref=dst, send_sem=ssem, recv_sem=rsem, device_id=dev, device_id_type=MESH_ID)

    def swap(kind, src_of, dst, mode):
        for k in range(1, num_tp):
            peer = lax.rem(rank + k, num_tp)
            if mode == 'recv':
                push(dst.at[peer], dst.at[peer], tp_send.at[kind, k], tp_recv.at[kind, peer], {'tp': rank}).wait_recv()
            else:
                copy = push(src_of(peer), dst.at[rank], tp_send.at[kind, k], tp_recv.at[kind, rank], {'tp': peer})
                copy.start() if mode == 'start' else copy.wait_send()

    num_x = num_pp // 2
    chip, core = stage // 2, lax.rem(stage, 2)
    partner = chip * 2 + 1 - core
    is_top = chip == num_x - 1
    is_lookup = stage == last - 1
    mirror = (num_x - 1 - chip) * 2 + core

    def tree(kind, tid, buf, root, mode):
        root_x, root_c = root // 2, root % 2
        on_core = core == root_c
        plus = lax.rem(chip + 1, num_x) * 2 + root_c
        minus = lax.rem(chip + num_x - 1, num_x) * 2 + root_c
        at_root = jnp.logical_and(on_core, chip == root_x)
        at_next = jnp.logical_and(on_core, jnp.logical_or(chip == root_x, chip == (root_x + 1) % num_x))
        for i in range(num_tp):
            blk = lax.rem(rank + i, num_tp)

            def go(slot, dest):
                copy = push(buf.at[blk], buf.at[blk], tree_send.at[tid, slot, i], tp_recv.at[kind, blk], {'pp': dest})
                copy.start() if mode == 'start' else copy.wait_send()

            if mode == 'start':
                wait = push(buf.at[blk], buf.at[blk], tree_send.at[tid, 0, i], tp_recv.at[kind, blk], {'pp': stage})
                if i == 0:
                    pl.when(stage != root)(wait.wait_recv)
                else:
                    wait.wait_recv()

            @pl.when(on_core)
            def _():
                go(2, partner)

            @pl.when(at_root)
            def _():
                go(0, minus)

            @pl.when(at_next)
            def _():
                go(1, plus)

    barrier = pltpu.get_barrier_semaphore()
    for k in range(1, num_tp):
        for pp in (stage, partner):
            pl.semaphore_signal(barrier, inc=1, device_id={'tp': lax.rem(rank + k, num_tp), 'pp': pp}, device_id_type=MESH_ID)
    for k in range(1, num_pp):
        pl.semaphore_signal(barrier, inc=1, device_id={'pp': lax.rem(stage + k, num_pp)}, device_id_type=MESH_ID)
    pl.semaphore_wait(barrier, 2 * (num_tp - 1) + num_pp - 1)

    own1 = pltpu.make_async_copy(w1_hbm, w1s.at[rank], loc.at[0])
    own2 = pltpu.make_async_copy(w2_hbm, w2s.at[rank], loc.at[1])
    own1.start()
    own2.start()

    rows_w = w1_hbm.shape[0]
    detours = [(0, rows_w * 3 // 8), (1, rows_w // 8)] if num_x >= 4 else []

    def w_copy(idx, rows=None):
        src, full, who, dev = [
            (w1_hbm, w1s, rank, right), (w2_hbm, w2s, rank, right), (w1_hbm, w1s, rank, left), (w2_hbm, w2s, rank, left),
            (w1s.at[left], w1s, left, right), (w2s.at[right], w2s, right, left)][idx]
        if rows is None:
            return push(src, full.at[who], w_send.at[idx], w_recv.at[idx], {'tp': dev})
        part = pl.ds(0, rows)
        return push(src.at[part], full.at[who, part], w_send.at[idx], w_recv.at[idx], {'tp': dev})

    def w_wait(idx, rows=None):
        full, who = [(w1s, left), (w2s, left), (w1s, right), (w2s, right), (w1s, opp), (w2s, opp)][idx]
        view = full.at[who] if rows is None else full.at[who, pl.ds(0, rows)]
        push(view, view, w_send.at[idx], w_recv.at[idx], {'tp': rank}).wait_recv()

    def by_chip(action):
        for near, size in detours:
            pl.when(chip == near)(functools.partial(action, rows_w - size))
        pl.when(chip >= len(detours))(functools.partial(action, None))

    def detour(size, leg, j):
        part = pl.ds(0, size)
        tail_rows = pl.ds(rows_w - size, size)
        if leg == 0:
            src = (w2_hbm, w1_hbm)[j].at[tail_rows]
            return push(src, via_x.at[j, part], via_send.at[j], via_recv.at[j], {'pp': mirror})
        if leg == 1:
            return push(via_x.at[j, part], via_y.at[j, part], via_send.at[2 + j], via_recv.at[2 + j], {'tp': (right, left)[j]})
        full, who = ((w2s, left), (w1s, right))[j]
        return push(via_y.at[j, part], full.at[who, tail_rows], via_send.at[4 + j], via_recv.at[4 + j], {'pp': mirror})

    def on_detour(helper, action):
        for near, size in detours:
            pl.when(chip == (num_x - 1 - near if helper else near))(functools.partial(action, size))

    w_copy(0).start()
    w_copy(3).start()

    def leave(size):
        for j in range(2):
            detour(size, 0, j).start()

    def pass_on(size):
        for j in range(2):
            detour(size, 0, j).wait_recv()
            detour(size, 1, j).start()

    def bring_back(size):
        for j in range(2):
            detour(size, 1, j).wait_recv()
            detour(size, 2, j).start()

    def arrive(size):
        for j in range(2):
            detour(size, 2, j).wait_recv()

    def second(rows):
        w_copy(1, rows).start()
        w_copy(2, rows).start()

    on_detour(False, leave)
    on_detour(True, pass_on)

    @pl.when(jnp.logical_not(is_lookup))
    def _():
        by_chip(second)

    def flip(src, dst, who):
        def one(j, carry):
            part = pl.ds(pl.multiple_of(j * 128, 128), 128)
            dst[who, :, part] = jnp.transpose(src[who, part, :])
            return carry
        lax.fori_loop(0, src.shape[1] // 128, one, 0)

    num_tok = num_tp * seq
    vocab_base = rank * vocab
    tail_base = (2 * half - 1) * tile
    tail = vocab - tail_base
    tok_row = tok[...] - vocab_base
    lab_row = lab[...] - vocab_base
    rows_in = lax.broadcasted_iota(jnp.int32, (chunk // 8, 8, num_tok), 0) * 8 + lax.broadcasted_iota(jnp.int32, (chunk // 8, 8, num_tok), 1)

    def at(i):
        return pl.multiple_of(i * tile, 16)

    def fetch(e_buf, base, size, slot):
        return pltpu.make_async_copy(e_hbm.at[pl.ds(base, size)], e_buf.at[slot, pl.ds(0, size)], loc.at[2 + slot])

    def sort_tokens():
        key_row = jnp.where(jnp.logical_and(tok_row >= 0, tok_row < vocab), tok_row, 1 << 20).astype(F32)
        lanes = lax.broadcasted_iota(jnp.int32, (1, num_tok), 1).astype(F32)
        step = 128
        key_buf[...] = jnp.transpose(jnp.broadcast_to(key_row, (step, num_tok)))

        def count(b, pos):
            here = key_buf[pl.ds(pl.multiple_of(b * step, step), step), 0:1]
            idx = (lax.broadcasted_iota(jnp.int32, (step, 1), 0) + b * step).astype(F32)
            ahead = jnp.logical_or(here < key_row, jnp.logical_and(here == key_row, idx < lanes))
            return pos + jnp.sum(jnp.where(ahead, 1.0, 0.0), axis=0, keepdims=True)

        def starts(b, acc):
            here = key_buf[pl.ds(pl.multiple_of(b * step, step), step), 0:1]
            return acc + jnp.sum(jnp.where(here < lanes * block, 1.0, 0.0), axis=0, keepdims=True)

        zero = jnp.zeros((1, num_tok), F32)
        pos_row = lax.fori_loop(0, num_tok // step, count, zero)
        offs = lax.fori_loop(0, num_tok // step, starts, zero)

        def place(b, carry):
            keys, idxs = carry
            here = key_buf[pl.ds(pl.multiple_of(b * step, step), step), 0:1]
            pos = key_buf[pl.ds(pl.multiple_of(b * step, step), step), 1:2]
            idx = (lax.broadcasted_iota(jnp.int32, (step, 1), 0) + b * step).astype(F32)
            mine = pos == lanes
            keys = keys + jnp.sum(jnp.where(mine, here, 0.0), axis=0, keepdims=True)
            return keys, idxs + jnp.sum(jnp.where(mine, idx, 0.0), axis=0, keepdims=True)

        both = jnp.where(lax.broadcasted_iota(jnp.int32, (step, num_tok), 0) == 0, key_row, pos_row)
        key_buf[...] = jnp.transpose(both)
        keys, idxs = lax.fori_loop(0, num_tok // step, place, (zero, zero))
        line = lax.broadcasted_iota(jnp.int32, (8, num_tok), 0)
        meta_o[...] = jnp.where(line == 0, keys, jnp.where(line == 1, idxs, offs)).astype(jnp.int32)

    sort_tokens()

    def lookup_pass(e_buf, acc):
        def tile_of(base, size, slot):
            def one(c, carry):
                row = base + c * chunk
                hot = jnp.where(rows_in == (tok_row - row)[None], 1.0, 0.0)
                g_buf[slot, pl.ds(pl.multiple_of(c * chunk, chunk), chunk), :] = hot.reshape(chunk, num_tok).astype(BF16)
                return carry
            lax.fori_loop(0, size // chunk, one, 0)
            fetch(e_buf, base, size, slot).wait()
            acc[...] += dot_of(g_buf[slot, pl.ds(0, size), :], e_buf[slot, pl.ds(0, size), :], 0, 0)

        acc[...] = jnp.zeros_like(acc)
        fetch(e_buf, 0, tile, 0).start()
        count = 2 * half - 1

        def one(i, carry):
            slot = lax.rem(i, 2)

            @pl.when(i + 1 < count)
            def _():
                fetch(e_buf, at(i + 1), tile, 1 - slot).start()
            tile_of(at(i), tile, slot)
            return carry
        lax.fori_loop(0, count, one, 0)
        fetch(e_buf, tail_base, tail, 0).start()
        tile_of(tail_base, tail, 0)
        for k in range(num_tp):
            x0[k] = acc[k * seq:(k + 1) * seq, :].astype(BF16)

    @pl.when(is_lookup)
    def _():
        pl.run_scoped(lookup_pass, pltpu.VMEM((2, tile, dim), BF16), pltpu.VMEM((num_tok, dim), F32))
        swap(X0, lambda peer: x0.at[peer], x0r, 'start')
        second(None)

    on_detour(True, bring_back)
    first_x = push(y_buf.at[pl.ds(1, 1)], x_in, p_send.at[5], p_recv.at[5], {'pp': 0})

    @pl.when(is_lookup)
    def _():
        swap(X0, None, x0r, 'recv')
        total = x0[rank].astype(F32)
        for k in range(1, num_tp):
            total = total + x0r[lax.rem(rank + k, num_tp)].astype(F32)
        y_buf[1] = total.astype(BF16)
        first_x.start()

    own1.wait()
    own2.wait()
    flip(w1s, w1t, rank)
    flip(w2s, w2t, rank)
    w_wait(0)
    w_copy(4).start()
    w_wait(3)
    w_copy(5).start()
    flip(w1s, w1t, left)
    flip(w2s, w2t, right)

    @pl.when(is_lookup)
    def _():
        first_x.wait_send()

    def second_in(rows):
        w_wait(1, rows)
        w_wait(2, rows)

    by_chip(second_in)
    on_detour(False, arrive)
    flip(w2s, w2t, left)
    flip(w1s, w1t, right)
    w_wait(4)
    w_wait(5)

    cols = w1s.shape[2]
    piece = 256 if cols % 256 == 0 and dim % 256 == 0 else 128
    cut = dim // 3 // 128 * 128
    spans = [(0, cut), (cut, dim - cut)] if cut else [(0, dim)]

    def hop(kind, src, dst, part, dest):
        lo, size = spans[part]
        view = (0, slice(None), pl.ds(lo, size))
        return push(src.at[view], dst.at[view], p_send.at[2 * kind + part], p_recv.at[2 * kind + part], {'pp': dest})

    def hops(kind, mode):
        src, dst = (y_buf.at[pl.ds(0, 1)], x_in) if kind == 0 else (y_buf.at[pl.ds(1, 1)], dy_in)
        dest = jnp.minimum(stage + 1, last) if kind == 0 else jnp.maximum(stage - 1, 0)
        return [hop(kind, src, dst, part, dest) for part in range(len(spans))]

    def send_rows(kind, source, acts, mats, active):
        for part, (lo, size) in enumerate(spans):
            for off in range(lo, lo + size, piece):
                total = source[0, :, off:off + piece].astype(F32)
                for blk in range(num_tp):
                    total = total + dot_of(acts[blk], mats[blk, :, off:off + piece], 1, 0)
                y_buf[kind, :, off:off + piece] = total.astype(BF16)

            @pl.when(active)
            def _():
                hops(kind, 'start')[part].start()

    @pl.when(jnp.logical_not(is_first))
    def _():
        for copy in hops(0, 'recv'):
            copy.wait_recv()

    @pl.when(is_first)
    def _():
        first_x.wait_recv()

    x_act = x_in[0]
    for blk in range(num_tp):
        for off in range(0, cols, piece):
            gate, grad = gelu_pair(dot_of(x_act, w1s[blk, :, off:off + piece], 1, 0))
            a_own[blk, :, off:off + piece] = gate.astype(BF16)
            slope[blk, :, off:off + piece] = grad
    send_rows(0, x_in, a_own, w2s, jnp.logical_not(is_last))

    def norm_of():
        wide = y_buf[0].astype(F32)
        inv_rms = lax.rsqrt(jnp.mean(wide * wide, axis=-1, keepdims=True) + NORM_EPS)
        return inv_rms, wide * inv_rms

    @pl.when(is_last)
    def _():
        n_all[rank] = norm_of()[1].astype(BF16)
        swap(N, lambda peer: n_all.at[rank], n_all, 'start')

    flip(w1s, w1t, opp)
    flip(w2s, w2t, opp)
    tree(N, 0, n_all, last, 'start')
    x_all[rank] = x_in[0]
    a_cols[rank] = a_own[rank]

    @pl.when(jnp.logical_not(is_top))
    def _():
        swap(XA, lambda peer: x_in.at[0], x_all, 'start')
        swap(AC, lambda peer: a_own.at[peer], a_cols, 'start')

    outs = [(n_all, n_o), (dx_all, dx_o), (x_all, xa_o), (a_cols, ac_o), (dy_all, dy_o), (dh_cols, dh_o)]

    def out_copy(idx):
        return pltpu.make_async_copy(outs[idx][0], outs[idx][1], out_sem.at[idx])

    out_copy(0).start()
    normed = n_all[...].reshape(num_tok, dim)
    base0 = core * (half * tile)
    mine = half - core
    is_odd = core == 1

    def stats_of(base, count, carry):
        def one(c, carry):
            top, acc, hit = carry
            row = pl.multiple_of(base + c * chunk, chunk)
            part = logit[pl.ds(row, chunk), :].reshape(chunk // 8, 8, num_tok)
            new = jnp.maximum(top, jnp.max(part, axis=0))
            acc = acc * jnp.exp(top - new) + jnp.sum(jnp.exp(part - new[None]), axis=0)
            hit = hit + jnp.sum(jnp.where(rows_in == (lab_row - (base0 + row))[None], part, 0.0), axis=0)
            return new, acc, hit
        return lax.fori_loop(0, count // chunk, one, carry)

    slot_of = rank * 2 + core

    def logits_pass(e_buf):
        def finish(carry):
            top, acc, hit = carry
            peak = jnp.max(top, axis=0, keepdims=True)
            total = jnp.sum(acc * jnp.exp(top - peak), axis=0, keepdims=True)
            hits = jnp.sum(hit, axis=0, keepdims=True)
            line = lax.broadcasted_iota(jnp.int32, (8, num_tok), 0)
            stat[slot_of] = jnp.where(line == 0, peak, jnp.where(line == 1, total, hits))

        def one(i, carry):
            slot = lax.rem(i, 2)

            @pl.when(i + 1 < mine)
            def _():
                fetch(e_buf, base0 + at(i + 1), tile, 1 - slot).start()
            fetch(e_buf, base0 + at(i), tile, slot).wait()
            logit[pl.ds(at(i), tile), :] = dot_of(e_buf[slot], normed, 1, 1)
            return stats_of(at(i), tile, carry)

        zero = jnp.zeros((8, num_tok), F32)
        fetch(e_buf, base0, tile, 0).start()
        carry = lax.fori_loop(0, mine, one, (jnp.full((8, num_tok), -jnp.inf, F32), zero, zero))

        @pl.when(is_odd)
        def _():
            slot = (half - 1) % 2
            fetch(e_buf, tail_base, tail, slot).start()
            fetch(e_buf, tail_base, tail, slot).wait()
            logit[pl.ds((half - 1) * tile, tail), :] = dot_of(e_buf[slot, pl.ds(0, tail), :], normed, 1, 1)
            finish(stats_of((half - 1) * tile, tail, carry))

        @pl.when(jnp.logical_not(is_odd))
        def _():
            finish(carry)

    pl.run_scoped(logits_pass, pltpu.VMEM((2, tile, dim), BF16))

    def stats_swap(mode):
        for k in range(num_tp):
            for flip in range(2):
                if k == 0 and flip == 0:
                    continue
                peer = lax.rem(rank + k, num_tp)
                peer_core = core if flip == 0 else 1 - core
                theirs = peer * 2 + peer_core
                if mode == 'recv':
                    push(stat.at[theirs], stat.at[theirs], st_send.at[2 * k + flip], st_recv.at[theirs], {'tp': rank}).wait_recv()
                else:
                    copy = push(stat.at[slot_of], stat.at[slot_of], st_send.at[2 * k + flip], st_recv.at[slot_of],
                                {'tp': peer, 'pp': chip * 2 + peer_core})
                    copy.start() if mode == 'start' else copy.wait_send()

    stats_swap('start')
    stats_swap('recv')

    @pl.when(is_top)
    def _():
        swap(XA, lambda peer: x_in.at[0], x_all, 'start')

    peak = stat[0, 0:1, :]
    for j in range(1, 2 * num_tp):
        peak = jnp.maximum(peak, stat[j, 0:1, :])
    total = jnp.zeros_like(peak)
    target = jnp.zeros_like(peak)
    for j in range(2 * num_tp):
        total = total + stat[j, 1:2, :] * jnp.exp(stat[j, 0:1, :] - peak)
        target = target + stat[j, 2:3, :]
    log_norm = peak + jnp.log(total)
    loss = jnp.sum(log_norm - target, axis=1, keepdims=True) / num_tok
    loss_o[...] = jnp.broadcast_to(loss, loss_o.shape)
    norm_rows = jnp.broadcast_to(log_norm, (8, num_tok))

    def grad_tile(base, count, slot):
        def one(c, carry):
            row = pl.multiple_of(base + c * chunk, chunk)
            part = logit[pl.ds(row, chunk), :].reshape(chunk // 8, 8, num_tok)
            hit = jnp.where(rows_in == (lab_row - (base0 + row))[None], 1.0, 0.0)
            part = jnp.exp(part - norm_rows[None]) - hit
            g_buf[slot, pl.ds(pl.multiple_of(c * chunk, chunk), chunk), :] = part.reshape(chunk, num_tok).astype(BF16)
            return carry
        lax.fori_loop(0, count // chunk, one, 0)

    def g_copies(i, base, size, slot):
        here, there = g_buf.at[slot, pl.ds(0, size)], g_o.at[pl.ds(base, size)]
        return pltpu.make_async_copy(here, there, loc.at[4 + slot]), push(here, there, g_send.at[slot], g_recv.at[i], {'pp': partner})

    def g_start(i, base, size, slot):
        for copy in g_copies(i, base, size, slot):
            copy.start()

    def g_wait(i, base, size, slot):
        keep, send = g_copies(i, base, size, slot)
        keep.wait()
        send.wait_send()

    def grads_pass(e_buf, dn_acc):
        @pl.when(is_top)
        def _():
            dn_acc[...] = jnp.zeros_like(dn_acc)
            fetch(e_buf, base0, tile, 0).start()

        def one(i, carry):
            slot = lax.rem(i, 2)

            @pl.when(i >= 2)
            def _():
                g_wait(i - 2, base0 + at(i - 2), tile, slot)
            grad_tile(at(i), tile, slot)
            g_start(i, base0 + at(i), tile, slot)

            @pl.when(is_top)
            def _():
                @pl.when(i + 1 < mine)
                def _():
                    fetch(e_buf, base0 + at(i + 1), tile, 1 - slot).start()
                fetch(e_buf, base0 + at(i), tile, slot).wait()
                dn_acc[...] += dot_of(g_buf[slot], e_buf[slot], 0, 0)
            return carry

        lax.fori_loop(0, mine, one, 0)
        final = half - 1
        slot = final % 2

        @pl.when(is_odd)
        def _():
            @pl.when(is_top)
            def _():
                fetch(e_buf, tail_base, tail, slot).start()
            if final >= 2:
                g_wait(final - 2, base0 + (final - 2) * tile, tile, slot)
            grad_tile(final * tile, tail, slot)
            g_start(final, tail_base, tail, slot)

            @pl.when(is_top)
            def _():
                fetch(e_buf, tail_base, tail, slot).wait()
                dn_acc[...] += dot_of(g_buf[slot, pl.ds(0, tail), :], e_buf[slot, pl.ds(0, tail), :], 0, 0)
        to_top = push(dn_send, dn_half, p_send.at[4], p_recv.at[4], {'pp': partner})

        @pl.when(jnp.logical_and(is_top, jnp.logical_not(is_last)))
        def _():
            for k in range(num_tp):
                dn_send[k] = dn_acc[k * seq:(k + 1) * seq, :].astype(BF16)
            to_top.start()

        @pl.when(is_last)
        def _():
            to_top.wait_recv()
            for k in range(num_tp):
                both = dn_acc[k * seq:(k + 1) * seq, :] + dn_half[k].astype(F32)
                dn_acc[k * seq:(k + 1) * seq, :] = both
                dn_send[k] = both.astype(BF16)
            swap(DN, lambda peer: dn_send.at[peer], dn_recv, 'start')
            swap(DN, None, dn_recv, 'recv')
            grad_n = dn_acc[pl.ds(pl.multiple_of(rank * seq, seq), seq), :]
            for k in range(1, num_tp):
                grad_n = grad_n + dn_recv[lax.rem(rank + k, num_tp)].astype(F32)
            inv_rms, unit = norm_of()
            dy_in[0] = (inv_rms * (grad_n - unit * jnp.mean(unit * grad_n, axis=-1, keepdims=True))).astype(BF16)

    pl.run_scoped(grads_pass, pltpu.VMEM((2, tile, dim), BF16), pltpu.VMEM((num_tok, dim), F32))

    @pl.when(jnp.logical_not(is_last))
    def _():
        for copy in hops(1, 'recv'):
            copy.wait_recv()

    dy_all[rank] = dy_in[0]
    swap(DY, lambda peer: dy_in.at[0], dy_all, 'start')
    grad_y = dy_in[0]
    for blk in range(num_tp):
        for off in range(0, cols, piece):
            grad_a = dot_of(grad_y, w2t[blk, :, off:off + piece], 1, 0)
            dh_own[blk, :, off:off + piece] = (slope[blk, :, off:off + piece] * grad_a).astype(BF16)
    send_rows(1, dy_in, dh_own, w1t, jnp.logical_not(is_first))

    @pl.when(is_top)
    def _():
        swap(AC, lambda peer: a_own.at[peer], a_cols, 'start')

    @pl.when(is_first)
    def _():
        dx_all[rank] = y_buf[1]
        swap(DX, lambda peer: y_buf.at[1], dx_all, 'start')

    dh_cols[rank] = dh_own[rank]

    @pl.when(chip != 0)
    def _():
        swap(DH, lambda peer: dh_own.at[peer], dh_cols, 'start')

    tree(DX, 1, dx_all, 0, 'start')

    @pl.when(chip == 0)
    def _():
        swap(DH, lambda peer: dh_own.at[peer], dh_cols, 'start')

    out_copy(1).start()
    for idx, kind, dst in ((2, XA, x_all), (3, AC, a_cols), (4, DY, dy_all), (5, DH, dh_cols)):
        swap(kind, None, dst, 'recv')
        out_copy(idx).start()

    for idx in (0, 3, 4, 5):
        w_copy(idx).wait_send()

    def second_sent(rows):
        w_copy(1, rows).wait_send()
        w_copy(2, rows).wait_send()

    def left_sent(size):
        for j in range(2):
            detour(size, 0, j).wait_send()

    def help_sent(size):
        for j in range(2):
            detour(size, 1, j).wait_send()
            detour(size, 2, j).wait_send()

    by_chip(second_sent)
    on_detour(False, left_sent)
    on_detour(True, help_sent)

    @pl.when(is_lookup)
    def _():
        swap(X0, lambda peer: x0.at[peer], x0r, 'sent')

    @pl.when(is_first)
    def _():
        swap(DX, lambda peer: y_buf.at[1], dx_all, 'sent')

    @pl.when(is_last)
    def _():
        swap(N, lambda peer: n_all.at[rank], n_all, 'sent')
        swap(DN, lambda peer: dn_send.at[peer], dn_recv, 'sent')

    @pl.when(jnp.logical_and(is_top, jnp.logical_not(is_last)))
    def _():
        push(dn_send, dn_half, p_send.at[4], p_recv.at[4], {'pp': partner}).wait_send()

    @pl.when(jnp.logical_not(is_last))
    def _():
        for copy in hops(0, 'sent'):
            copy.wait_send()

    @pl.when(jnp.logical_not(is_first))
    def _():
        for copy in hops(1, 'sent'):
            copy.wait_send()
    swap(XA, lambda peer: x_in.at[0], x_all, 'sent')
    swap(AC, lambda peer: a_own.at[peer], a_cols, 'sent')
    swap(DY, lambda peer: dy_in.at[0], dy_all, 'sent')
    swap(DH, lambda peer: dh_own.at[peer], dh_cols, 'sent')
    stats_swap('sent')
    tree(N, 0, n_all, last, 'sent')
    tree(DX, 1, dx_all, 0, 'sent')

    final = half - 1
    their_base = (1 - core) * (half * tile)

    @pl.when(is_odd)
    def _():
        if final >= 1:
            g_wait(final - 1, base0 + (final - 1) * tile, tile, (final - 1) % 2)
        g_wait(final, tail_base, tail, final % 2)

    @pl.when(jnp.logical_not(is_odd))
    def _():
        for i in range(max(final - 1, 0), half):
            g_wait(i, base0 + i * tile, tile, i % 2)
    for i in range(final):
        g_copies(i, their_base + i * tile, tile, i % 2)[1].wait_recv()

    @pl.when(is_odd)
    def _():
        g_copies(final, their_base + final * tile, tile, final % 2)[1].wait_recv()

    @pl.when(jnp.logical_not(is_odd))
    def _():
        g_copies(final, tail_base, tail, final % 2)[1].wait_recv()
    for idx in range(6):
        out_copy(idx).wait()


def table_kernel(block, meta, loss_in, n_all, dx_all, g_ref, xa, ac, dy, dh, loss_o, out_ref, dw1_o, dw2_o, dx_wide, acts, dw, sems):
    i = pl.program_id(0)
    num_tok, dim = dx_all.shape
    loads = [pltpu.make_async_copy(src, acts.at[j], sems.at[j]) for j, src in enumerate((ac, dy, xa, dh))]
    stores = [pltpu.make_async_copy(dw.at[j], dst, sems.at[4 + j]) for j, dst in enumerate((dw2_o, dw1_o))]

    @pl.when(i == 0)
    def _():
        for load in loads:
            load.start()
        dx_wide[...] = dx_all[...].astype(F32)
        loss_o[0] = jnp.max(loss_in[...])

    out_ref[...] = dot_of(g_ref[...], n_all[...], 1, 0)

    def add(k, carry):
        row = meta[0, k] - i * block
        out_ref[pl.ds(row, 1), :] += dx_wide[pl.ds(meta[1, k], 1), :]
        return carry
    lax.fori_loop(meta[2, i], meta[2, i + 1], add, 0)

    for j in range(2):
        @pl.when(i == 1 + j)
        def _():
            loads[2 * j].wait()
            loads[2 * j + 1].wait()
            dw[j] = dot_of(acts[2 * j], acts[2 * j + 1], 0, 0)
            stores[j].start()

    @pl.when(i == pl.num_programs(0) - 1)
    def _():
        for store in stores:
            store.wait()


def solution(mesh):
    num_tp, num_pp = mesh.shape['tp'], mesh.shape['pp']

    def device_fn(tokens, labels, emb_table, w_in, w_out):
        num_micro, seq = tokens.shape
        vocab, dim = emb_table.shape
        cols = w_in.shape[2]
        num_tok = num_micro * seq
        chunk = row_chunk(vocab)
        chunks = vocab // chunk
        half = 6 if chunks >= 60 else 2
        tile = chunk * pl.cdiv(chunks, 2 * half)
        block = min(640, tile)
        vmem, hbm = pl.BlockSpec(memory_space=pltpu.VMEM), pl.BlockSpec(memory_space=pl.ANY)
        act = (num_tp, seq, dim)
        wide = (num_tp, seq, cols)
        shape = jax.ShapeDtypeStruct
        dma = pltpu.SemaphoreType.DMA
        loss, meta, g_all, n_all, dx_all, x_all, a_cols, dy_all, dh_cols = pl.pallas_call(
            functools.partial(step_kernel, num_tp, num_pp, tile, half, block),
            out_shape=(shape((8, 128), F32), shape((8, num_tok), jnp.int32), shape((vocab, num_tok), BF16),
                       shape(act, BF16), shape(act, BF16), shape(act, BF16), shape(wide, BF16), shape(act, BF16), shape(wide, BF16)),
            in_specs=[vmem, vmem, hbm, hbm, hbm],
            out_specs=(vmem, vmem, hbm, hbm, hbm, hbm, hbm, hbm, hbm),
            scratch_shapes=[
                pltpu.VMEM(act, BF16), pltpu.VMEM(act, BF16), pltpu.VMEM((num_tp, dim, cols), BF16), pltpu.VMEM((num_tp, cols, dim), BF16),
                pltpu.VMEM((num_tp, cols, dim), BF16), pltpu.VMEM((num_tp, dim, cols), BF16),
                pltpu.VMEM((1, seq, dim), BF16), pltpu.VMEM((2, seq, dim), BF16), pltpu.VMEM(wide, BF16), pltpu.VMEM(wide, F32),
                pltpu.VMEM(act, BF16), pltpu.VMEM(act, BF16), pltpu.VMEM(wide, BF16), pltpu.VMEM(act, BF16), pltpu.VMEM(wide, BF16),
                pltpu.VMEM(wide, BF16), pltpu.VMEM((1, seq, dim), BF16), pltpu.VMEM(act, BF16),
                pltpu.VMEM((half * tile, num_tok), F32), pltpu.VMEM((2 * num_tp, 8, num_tok), F32),
                pltpu.VMEM(act, BF16), pltpu.VMEM(act, BF16), pltpu.VMEM(act, BF16),
                pltpu.VMEM((2, tile, num_tok), BF16), pltpu.VMEM((num_tok, 128), F32),
                pltpu.VMEM((2, dim // 2, dim), BF16), pltpu.VMEM((2, dim // 2, dim), BF16),
                dma((6,)), dma((6,)), dma((6,)), dma((6,)), dma((8, num_tp)), dma((8, num_tp)), dma((2, 3, num_tp)),
                dma((2 * num_tp,)), dma((2 * num_tp,)), dma((2,)), dma((half,)), dma((6,)), dma((6,)), dma((6,)), dma((6,)),
            ],
            compiler_params=pltpu.CompilerParams(collective_id=0, has_side_effects=True, vmem_limit_bytes=67043328),
            name='step_kernel',
        )(tokens.reshape(1, num_tok), labels.reshape(1, num_tok), emb_table, w_in[0], w_out[0])

        whole = lambda shp: pl.BlockSpec(shp, lambda i, meta: (0, 0))
        flat = lambda arr: arr.reshape(num_tok, arr.shape[2])
        loss, grad_table, grad_one, grad_two = pl.pallas_call(
            functools.partial(table_kernel, block),
            grid_spec=pltpu.PrefetchScalarGridSpec(
                num_scalar_prefetch=1,
                grid=(pl.cdiv(vocab, block),),
                in_specs=[whole((8, 128)), whole((num_tok, dim)), whole((num_tok, dim)), pl.BlockSpec((block, num_tok), lambda i, meta: (i, 0)), hbm, hbm, hbm, hbm],
                out_specs=(pl.BlockSpec(memory_space=pltpu.SMEM), pl.BlockSpec((block, dim), lambda i, meta: (i, 0)), hbm, hbm),
                scratch_shapes=[pltpu.VMEM((num_tok, dim), F32), pltpu.VMEM((4, num_tok, dim), BF16), pltpu.VMEM((2, dim, dim), F32), dma((6,))],
            ),
            out_shape=(shape((1,), F32), shape((vocab, dim), F32), shape((dim, cols), F32), shape((cols, dim), F32)),
            compiler_params=pltpu.CompilerParams(dimension_semantics=('arbitrary',), vmem_limit_bytes=67043328),
            name='table_kernel',
        )(meta, loss, flat(n_all), flat(dx_all), g_all, flat(x_all), flat(a_cols), flat(dy_all), flat(dh_cols))
        return loss, grad_one[None], grad_two[None], grad_table

    return jax.shard_map(device_fn, mesh=mesh, in_specs=(P('dp', None), P('dp', None), P('tp', None), P('pp', None, 'tp'), P('pp', 'tp', None)), out_specs=(P('dp'), P(('dp', 'pp'), None, 'tp'), P(('dp', 'pp'), 'tp', None), P(('dp', 'tp'), None)), check_vma=False)
```
